256 devices in a mesh: toa: 128 (over z, y, x), rep: 2 (over core).
Axes of the slice: x: 4, y: 4, z: 8, core: 2. Of those that a mesh axis runs over, the one named last changes fastest.
Arguments:
- residual: float32 [16384, 256], P('toa'), may hold values from -6 to 6
- toa_error: float32 [16384, 256], P('toa'), may hold values from 0.3 to 3
- basis_rows: bfloat16 [16384, 100, 256], P('toa', 'rep'), may hold values from -0.041432038 to 0.041432038
- efac_table: float32 [128, 64], replicated, may hold values from 0.5 to 2
- equad_table: float32 [128, 64], replicated, may hold values from 0.1 to 1
- pulsar: int32 [16384], P('toa'), may hold values from 0 to 127
- backend: int32 [16384], P('toa'), may hold values from 0 to 63
- counts: int32 [16384], P('toa'), may hold values from 64 to 256
- owner_slot: int32 [16384], P('toa'), may hold values from 0 to 16383, as said below
Outputs:
- gram_matrix: float32 [128, 100, 100], P('toa', None, 'rep')
- projection: float32 [128, 100], P('toa', 'rep')
- whitened: float32 [16384, 256], P('toa')
The draws below stay inside these ranges and needn't reach their ends.
Inputs may be any that keep to these rules, and one draw needn't show every extreme that they name: A permutation of the 16384 slots, independent of pulsar and backend; owner_slot // 128 is the device index along toa that holds the tile's output row and owner_slot % 128 its place there; each device's tiles go exactly 1 to each device.
All inputs are finite; a program needn't handle non-finite values.
Results may differ from the reference program's by a relative error of at most 0.0032.
Values may be sent and summed in bfloat16 or wider, within the bound.
No kernel may reach another device: no remote copies, remote signals or barrier semaphores. Data moves between devices by JAX's collectives and lax.ppermute only.
A program may use at most 64 MiB of HBM per device.

```python
import math
import jax
import jax.numpy as jnp
import numpy as np
from jax import lax

K = 100
B = 64
ROWS = 256
TILES_DEV = 128
PSR_DEV = 1
P_SIZE = 128
TILES = 16384


def draw_basis_rows(key, part):
    noise_key, column_key = jax.random.split(jax.random.fold_in(key, 11))
    spread = 1.0 / math.sqrt(TILES_DEV * ROWS // PSR_DEV)
    noise = jnp.clip(jax.random.normal(noise_key, (TILES, K, ROWS), jnp.float32), -6.0, 6.0)
    column_mean = jax.random.uniform(column_key, (K,), jnp.float32, -1.0, 1.0)
    values = (noise + column_mean[None, :, None]) * spread
    return values.astype(jnp.bfloat16)


def draw_owner_slot(key, part):
    source_key, dest_key = jax.random.split(jax.random.fold_in(key, 23))
    peer_count = TILES // TILES_DEV
    per_peer = TILES_DEV // peer_count
    source_order = jax.vmap(lambda small_key: jax.random.permutation(small_key, TILES_DEV))(jax.random.split(source_key, peer_count))
    dest_order = jax.vmap(lambda small_key: jax.random.permutation(small_key, TILES_DEV))(jax.random.split(dest_key, peer_count))
    source_ids = jnp.arange(peer_count, dtype=jnp.int32)[:, None, None]
    dest_ids = jnp.arange(peer_count, dtype=jnp.int32)[None, :, None]
    copy_ids = jnp.arange(per_peer, dtype=jnp.int32)[None, None, :]
    tile_index = source_ids * TILES_DEV + source_order[source_ids, dest_ids * per_peer + copy_ids]
    slot_value = dest_ids * TILES_DEV + dest_order[dest_ids, source_ids * per_peer + copy_ids]
    tile_index = jnp.broadcast_to(tile_index, (peer_count, peer_count, per_peer)).reshape(-1)
    slot_value = jnp.broadcast_to(slot_value, (peer_count, peer_count, per_peer)).reshape(-1)
    return jnp.zeros((TILES,), jnp.int32).at[tile_index].set(slot_value.astype(jnp.int32))


def touch_ends(array, stream_key, low, top_value):
    spot = [jax.random.randint(jax.random.fold_in(stream_key, axis), (), 0, length) for axis, length in enumerate(array.shape)]
    longest = array.shape.index(max(array.shape))
    next_to = spot[:longest] + [(spot[longest] + 1) % array.shape[longest]] + spot[longest + 1:]
    return array.at[tuple(spot)].set(low).at[tuple(next_to)].set(top_value)


def level_of(key, shape, cuts, smallest, top_value):
    factor_of = 1.0
    for position, blocks in cuts:
        heights = jax.random.uniform(jax.random.fold_in(jax.random.fold_in(key, 6), position), (blocks,), jnp.float32, smallest / len(cuts), top_value / len(cuts))
        factor_of = factor_of * jnp.repeat(jnp.exp(heights), shape[position] // blocks).reshape((-1,) + (1,) * (len(shape) - 1 - position))
    return factor_of


def cumulative_ranks(amount, slope):
    portions = [(1 << 20) // math.isqrt(standing ** slope) + 1 for standing in range(1, amount + 1)]
    width = 1 + sum(portions) // (1 << 30)
    return np.cumsum(np.array([max(1, weight // width) for weight in portions]))


def ranked(stream_key, extent, amount, skew):
    grid = cumulative_ranks(amount, skew)
    pick = jax.random.randint(jax.random.fold_in(stream_key, 1), extent, 0, int(grid[amount - 1]))
    grade = jnp.searchsorted(jnp.asarray(grid, jnp.int32), pick, side="right")
    return jax.random.permutation(jax.random.fold_in(stream_key, 2), amount)[grade].astype(jnp.int32)


def scatter_about(own_key, shape, width, most, cuts=(), kind=jnp.bfloat16):
    loudness = level_of(own_key, shape, cuts, -0.22, 0.18) if cuts else 1.0
    result = jax.random.normal(own_key, shape, jnp.float32) * width * loudness
    return jnp.minimum(jnp.maximum(result, -most), most).astype(kind)


def setup_inputs(seed: int = 0) -> dict:
    splits = jax.random.split(jax.random.key(seed), 10)
    residual = scatter_about(splits[0], (TILES, ROWS), 1.0, 6.0, ((0, 128),), jnp.float32)
    toa_error = jnp.clip(jnp.exp(math.log(3.0) - 2.3025851 * jax.random.uniform(splits[1], (TILES, ROWS), jnp.float32) ** level_of(splits[1], (TILES, ROWS), ((0, 128),), -0.2, 0.2)), 0.3, 3.0)
    basis_rows = draw_basis_rows(jax.random.fold_in(splits[9], 71), 0)
    efac_table = jnp.clip(jnp.exp(jax.random.uniform(splits[3], (P_SIZE, B), jnp.float32, math.log(0.5), math.log(2.0))), 0.5, 2.0)
    equad_table = jnp.clip(jnp.exp(jax.random.uniform(splits[4], (P_SIZE, B), jnp.float32, math.log(0.1), math.log(1.0))), 0.1, 1.0)
    pulsar = touch_ends(ranked(splits[5], (TILES,), P_SIZE, 1), jax.random.fold_in(splits[5], 3), 0, P_SIZE - 1).astype(jnp.int32)
    backend = touch_ends(jax.random.randint(splits[6], (TILES,), 0, B), jax.random.fold_in(splits[6], 1), 0, B - 1).astype(jnp.int32)
    counts = touch_ends(jax.random.randint(splits[7], (TILES,), ROWS // 4, ROWS + 1), jax.random.fold_in(splits[7], 1), ROWS // 4, ROWS).astype(jnp.int32)
    owner_slot = draw_owner_slot(jax.random.fold_in(splits[9], 71), 0)
    return {"residual": residual, "toa_error": toa_error, "basis_rows": basis_rows, "efac_table": efac_table, "equad_table": equad_table, "pulsar": pulsar, "backend": backend, "counts": counts, "owner_slot": owner_slot}


def reference(residual, toa_error, basis_rows, efac_table, equad_table, pulsar, backend, counts, owner_slot):
    factor = efac_table[pulsar, backend]
    floor_term = equad_table[pulsar, backend]
    valid_rows = jnp.arange(ROWS, dtype=jnp.int32)[None, :] < counts[:, None]
    weight = jnp.where(valid_rows, 1.0 / (factor[:, None] ** 2 * toa_error ** 2 + floor_term[:, None] ** 2), 0.0).astype(jnp.float32)
    whitened_local = jnp.sqrt(weight) * residual
    whitened = jnp.zeros_like(whitened_local).at[owner_slot.astype(jnp.int32)].set(whitened_local)
    block_count = TILES // TILES_DEV
    basis_blocks = basis_rows.reshape(block_count, TILES_DEV, K, ROWS)
    weight_blocks = weight.reshape(block_count, TILES_DEV, ROWS)
    residual_blocks = residual.reshape(block_count, TILES_DEV, ROWS)
    pulsar_blocks = pulsar.reshape(block_count, TILES_DEV)
    high = lax.Precision.HIGHEST

    def step_fn(carry, inputs):
        gram_sum, proj_sum = carry
        basis_block, weight_block, residual_block, pulsar_block = inputs
        basis_float = basis_block.astype(jnp.float32)
        scaled = lax.optimization_barrier((weight_block[:, None, :] * basis_float).astype(jnp.bfloat16)).astype(jnp.float32)
        weighted_res = lax.optimization_barrier((weight_block * residual_block).astype(jnp.bfloat16)).astype(jnp.float32)
        tile_gram = jnp.einsum('tkr,tjr->tkj', basis_float, scaled, precision=high)
        tile_proj = jnp.einsum('tkr,tr->tk', basis_float, weighted_res, precision=high)
        onehot = (pulsar_block[:, None] == jnp.arange(P_SIZE, dtype=jnp.int32)[None, :]).astype(jnp.float32)
        gram_sum = gram_sum + jnp.einsum('tp,tkj->pkj', onehot, tile_gram, precision=high)
        proj_sum = proj_sum + jnp.einsum('tp,tk->pk', onehot, tile_proj, precision=high)
        return ((gram_sum, proj_sum), None)
    initial = (jnp.zeros((P_SIZE, K, K), jnp.float32), jnp.zeros((P_SIZE, K), jnp.float32))
    (gram_matrix, projection), unused = lax.scan(step_fn, initial, (basis_blocks, weight_blocks, residual_blocks, pulsar_blocks))
    return (gram_matrix, projection, whitened)
```

```python
import functools

import jax
import jax.numpy as jnp
from jax import lax
from jax.experimental import pallas as pl
from jax.experimental.pallas import tpu as pltpu
from jax.sharding import Mesh
from jax.sharding import PartitionSpec as P

TOA = ("toa_0", "toa_1", "toa_2")
FAR, NEAR = "toa_0", ("toa_1", "toa_2")
BF16, F32 = jnp.bfloat16, jnp.float32
LANES = 128
HALF = 64
GROUP = 16
HEAD = 24
WHITE = 32


def dot(a, b, **kw):
    return lax.dot_general(a, b, (((1,), (0,)), ((), ())), preferred_element_type=F32, **kw)


def iota(shape, dim):
    return lax.broadcasted_iota(jnp.int32, shape, dim)


def as_column(row, lanes):
    square = jnp.broadcast_to(row, (LANES, row.shape[1])).T
    return jnp.concatenate([square] * (lanes // LANES), axis=1)


def gram_kernel(
    near, far, pulsar_sm, residual, error, efac_t, equad_t, pulsar, backend, counts, slot,
    own, other, out, acc, weight_vm, wres_vm,
):
    cols, tiles, rows = own.shape
    message = out.shape[1]
    pulsars, backends = efac_t.shape[1], efac_t.shape[0]

    of_pulsar = (iota((pulsars, tiles), 0) == pulsar[...]).astype(F32)
    of_backend = (iota((backends, tiles), 0) == backend[...]).astype(F32)
    high = dict(precision=lax.Precision.HIGHEST)
    factor = jnp.sum(dot(efac_t[...], of_pulsar, **high) * of_backend, axis=0, keepdims=True)
    floor = jnp.sum(dot(equad_t[...], of_pulsar, **high) * of_backend, axis=0, keepdims=True)
    factor2 = as_column(factor * factor, rows)
    floor2 = as_column(floor * floor, rows)
    count = as_column(counts[...].astype(F32), rows)
    valid = iota((tiles, rows), 1).astype(F32) < count
    weight = jnp.where(valid, 1.0 / (factor2 * error[...] ** 2 + floor2), 0.0)
    weight_vm[...] = weight
    wres_vm[...] = (weight * residual[...]).astype(BF16)
    white = (jnp.sqrt(weight) * residual[...]).astype(BF16)

    dest = slot[...] // tiles
    place = (slot[...] % tiles).astype(F32)
    order = (dest % near) * far + dest // near
    moved = (iota((tiles, tiles), 0) == order).astype(BF16)
    white_to = dot(moved, white)
    place_to = dot(moved, as_column(place, LANES).astype(BF16))
    acc[...] = jnp.zeros_like(acc)
    for n in range(near):
        at = n * message
        acc[at : at + far, :] = white_to[n * far : (n + 1) * far, :LANES]
        acc[at + far : at + 2 * far, :] = white_to[n * far : (n + 1) * far, LANES:]
        acc[at + 2 * far : at + 3 * far, :] = place_to[n * far : (n + 1) * far, :]

    def turn(g, carry):
        t0 = pl.multiple_of(g * GROUP, GROUP)
        mine = own[:, pl.ds(t0, GROUP), :]
        extra = wres_vm[pl.ds(t0, GROUP), :].reshape(1, GROUP, rows)
        mine = pltpu.einshape("ktr->tkr", jnp.concatenate([mine, extra], axis=0))
        theirs = pltpu.einshape("ktr->tkr", other[:, pl.ds(t0, GROUP), :])
        group_weight = weight_vm[pl.ds(t0, GROUP), :]
        for u in range(GROUP):
            left = mine[u]
            wrow = group_weight[u : u + 1, :]
            scaled = (left.astype(F32) * wrow).astype(BF16)
            scaled = jnp.where(iota(left.shape, 0) < cols, scaled, left)
            right = lambda a: lax.dot_general(
                a, scaled, (((1,), (1,)), ((), ())), preferred_element_type=F32
            )
            p = pulsar_sm[t0 + u]
            base = (p % near) * message + HEAD + (p // near) * cols
            acc[pl.ds(base, cols), : cols + 1] += right(left)[:cols]
            acc[pl.ds(base, cols), HALF : HALF + cols + 1] += right(theirs[u])
        return carry

    lax.fori_loop(0, tiles // GROUP, turn, 0)

    def pack(n, carry):
        at = pl.multiple_of(n * message, 8)
        value = acc[pl.ds(at, message), :]
        rest = value - value.astype(BF16).astype(F32)
        rest = pltpu.roll(rest, 1, 1)
        lane, row = iota(value.shape, 1), iota(value.shape, 0)
        value = jnp.where((lane == cols + 1) & (row >= HEAD), rest, value)
        out[n] = value.astype(BF16)
        return carry

    lax.fori_loop(0, near, pack, 0)


def near_kernel(far, cols, got, out, total):
    near = got.shape[0]
    for half in range(2):
        part = got[:, half * far : (half + 1) * far, :].astype(F32)
        out[:, half * near : (half + 1) * near, :] = jnp.swapaxes(part, 0, 1).astype(BF16)
    place = jnp.zeros((far, LANES), F32)
    lane = iota((far, LANES), 1)
    summed = got[0, HEAD:, :].astype(F32)
    for n in range(near):
        place = jnp.where(lane == n, got[n, 2 * far : 3 * far, :].astype(F32), place)
        if n:
            summed = summed + got[n, HEAD:, :].astype(F32)
    total[: far * cols, :] = summed
    total[far * cols :, :] = place
    for f in range(far):
        out[f, WHITE : WHITE + cols, :] = total[f * cols : (f + 1) * cols, :].astype(BF16)
        out[f, WHITE + cols :, :] = jnp.broadcast_to(
            total[far * cols + f : far * cols + f + 1, :], (out.shape[1] - WHITE - cols, LANES)
        ).astype(BF16)


def far_kernel(cols, got, core, gram, proj, white):
    far, near = got.shape[0], WHITE // 2
    tiles = far * near
    place = jnp.zeros((1, LANES), F32)
    lane = iota((1, LANES), 1)
    total = jnp.zeros((got.shape[1] - WHITE, LANES), F32)
    for f in range(far):
        part = got[f, WHITE:, :].astype(F32)
        total = total + part
        row = part[cols : cols + 1, :]
        row = pltpu.roll(row, f * near, 1) if f else row
        place = jnp.where(lane // near == f, row, place)
    total = jnp.concatenate([total, jnp.zeros((LANES - total.shape[0], LANES), F32)], axis=0)
    turned = total.T
    mine = turned[:cols]
    theirs = turned[HALF : HALF + cols]
    first = core[0] == 0
    low = jnp.where(first, mine, theirs)
    high = jnp.where(first, theirs, mine)
    both = jnp.where(iota(low.shape, 1) < cols, low, pltpu.roll(high, cols, 1))
    gram[...] = both[:, : 2 * cols]
    proj[...] = (turned[cols : cols + 1] + turned[cols + 1 : cols + 2])[:, :cols]
    put = (iota((tiles, tiles), 0) == place.astype(jnp.int32)).astype(BF16)
    for half in range(2):
        rows = got[:, half * near : (half + 1) * near, :].reshape(tiles, LANES)
        white[:, half * LANES : (half + 1) * LANES] = dot(put, rows)


def vmem(n):
    return [pl.BlockSpec(memory_space=pltpu.VMEM)] * n


SMEM = pl.BlockSpec(memory_space=pltpu.SMEM)


def shards(
    residual, toa_error, basis_rows, efac_table, equad_table, pulsar, backend, counts, owner_slot
):
    far, near = lax.axis_size(FAR), lax.axis_size(NEAR)
    tiles, cols, rows = basis_rows.shape
    own = jnp.transpose(basis_rows, (1, 0, 2))
    other = lax.ppermute(own, "rep", [(0, 1), (1, 0)])
    message = HEAD + far * cols
    line = lambda a: a.reshape(1, -1)
    sent = pl.pallas_call(
        functools.partial(gram_kernel, near, far),
        out_shape=jax.ShapeDtypeStruct((near, message, LANES), BF16),
        in_specs=[SMEM] + vmem(10),
        out_specs=vmem(1)[0],
        scratch_shapes=[
            pltpu.VMEM((near * message, LANES), F32),
            pltpu.VMEM((tiles, rows), F32),
            pltpu.VMEM((tiles, rows), BF16),
        ],
        compiler_params=pltpu.CompilerParams(vmem_limit_bytes=40 << 20),
        name="gram",
    )(
        pulsar, residual, toa_error, efac_table.T, equad_table.T, line(pulsar), line(backend),
        line(counts), line(owner_slot), own, other,
    )
    got = lax.all_to_all(sent, NEAR, 0, 0, tiled=True)
    far_rows = WHITE + cols + 8 - (WHITE + cols) % 8
    sent = pl.pallas_call(
        functools.partial(near_kernel, far, cols),
        out_shape=jax.ShapeDtypeStruct((far, far_rows, LANES), BF16),
        in_specs=vmem(1),
        out_specs=vmem(1)[0],
        scratch_shapes=[pltpu.VMEM((far * cols + far, LANES), F32)],
        name="near_sum",
    )(got)
    got = lax.all_to_all(sent, FAR, 0, 0, tiled=True)
    core = lax.axis_index("rep").reshape(1)
    gram, projection, whitened = pl.pallas_call(
        functools.partial(far_kernel, cols),
        out_shape=(
            jax.ShapeDtypeStruct((cols, 2 * cols), F32),
            jax.ShapeDtypeStruct((1, cols), F32),
            jax.ShapeDtypeStruct((tiles, rows), F32),
        ),
        in_specs=vmem(1) + [SMEM],
        out_specs=tuple(vmem(3)),
        name="far_sum",
    )(got, core)
    return gram.T[None], projection, whitened


def solution(mesh):
    split = Mesh(
        mesh.devices.reshape(8, 4, 4, mesh.shape["rep"]), ("toa_0", "toa_1", "toa_2", "rep")
    )
    placed = (
        P(TOA, None),
        P(TOA, None),
        P(TOA, "rep", None),
        P(),
        P(),
        P(TOA),
        P(TOA),
        P(TOA),
        P(TOA),
    )
    return jax.shard_map(
        shards,
        mesh=split,
        in_specs=placed,
        out_specs=(P(TOA, None, "rep"), P(TOA, "rep"), P(TOA, None)),
        check_vma=False,
    )
```

```python
import functools

import jax
import jax.numpy as jnp
from jax import lax
from jax.experimental import pallas as pl
from jax.experimental.pallas import tpu as pltpu
from jax.sharding import Mesh
from jax.sharding import PartitionSpec as P

TOA = ("toa_0", "toa_1", "toa_2")
FAR, NEAR = "toa_0", ("toa_1", "toa_2")
BF16, F32 = jnp.bfloat16, jnp.float32
LANES = 128
GROUP = 16

PART = 25
WIDE = PART + 1
SECOND = 32
DIAGONAL = ((0, 7, 25), (7, 13, 58), (13, 25, 64))
CROSS = 76
PLACE = 126
WHITE = 32


def dot(a, b, dims=((1,), (0,)), **kw):
    return lax.dot_general(a, b, (dims, ((), ())), preferred_element_type=F32, **kw)


def iota(shape, dim):
    return lax.broadcasted_iota(jnp.int32, shape, dim)


def as_column(row, lanes):
    square = jnp.broadcast_to(row, (LANES, row.shape[1])).T
    return jnp.concatenate([square] * (lanes // LANES), axis=1)


def base_row(p, near, message, head):
    return (p % near) * message + head + (p // near) * WIDE


def own_kernel(
    near, far, pulsar_in, backend_in, counts_in, slot_in, residual_in, error_in, efac_in, equad_in,
    own_in, left_out, acc,
    pulsar, backend, counts, slot, residual, error, efac_t, equad_t, own, pulsar_sm,
    weight_vm, wres_vm, sems,
):
    cols, tiles, rows = own.shape
    head = 2 * far
    message = head + far * WIDE
    pulsars, backends = efac_t.shape[1], efac_t.shape[0]
    pairs = (
        (pulsar_in, pulsar), (backend_in, backend), (counts_in, counts), (slot_in, slot),
        (residual_in, residual), (error_in, error), (efac_in, efac_t), (equad_in, equad_t),
        (pulsar_in, pulsar_sm), (own_in, own),
    )
    copies = [pltpu.make_async_copy(a, b, sems.at[i]) for i, (a, b) in enumerate(pairs)]
    for copy in copies:
        copy.start()
    acc[...] = jnp.zeros_like(acc)
    for copy in copies[:-1]:
        copy.wait()

    of_pulsar = (iota((pulsars, tiles), 0) == pulsar[...]).astype(F32)
    of_backend = (iota((backends, tiles), 0) == backend[...]).astype(F32)
    high = dict(precision=lax.Precision.HIGHEST)
    factor = jnp.sum(dot(efac_t[...], of_pulsar, **high) * of_backend, axis=0, keepdims=True)
    floor = jnp.sum(dot(equad_t[...], of_pulsar, **high) * of_backend, axis=0, keepdims=True)
    factor2 = as_column(factor * factor, rows)
    floor2 = as_column(floor * floor, rows)
    count = as_column(counts[...].astype(F32), rows)
    valid = iota((tiles, rows), 1).astype(F32) < count
    weight = jnp.where(valid, 1.0 / (factor2 * error[...] ** 2 + floor2), 0.0)
    weight_vm[...] = weight
    wres_vm[...] = (weight * residual[...]).astype(BF16)
    white = (jnp.sqrt(weight) * residual[...]).astype(BF16)

    me = lax.axis_index("toa_1") * lax.axis_size("toa_2") + lax.axis_index("toa_2")
    dest = slot[...] // tiles
    place = (slot[...] % tiles).astype(F32)
    order = (dest % near) * far + dest // near
    moved = (iota((tiles, tiles), 0) == order).astype(BF16)
    white_to = dot(moved, white)
    place_to = dot(moved, as_column(place, LANES).astype(BF16))
    place_to = jnp.where(iota(place_to.shape, 1) == PLACE, place_to, 0.0)
    for n in range(near):
        at = n * message
        acc[at : at + far, :] = white_to[n * far : (n + 1) * far, :LANES]
        acc[at + far : at + 2 * far, :] = white_to[n * far : (n + 1) * far, LANES:]
        acc[pl.ds(at + head + me, far, stride=WIDE), :] = place_to[n * far : (n + 1) * far, :]
    copies[-1].wait()

    lefts = 2 * SECOND
    wide = 80
    lane, row = iota((SECOND, wide), 1), iota((SECOND, wide), 0)
    own_lane = (lane < PART) | ((lane >= SECOND) & (lane < SECOND + PART))
    second = (~own_lane) | (row == PART)
    kept = own_lane | (row != PART)
    is_wres = iota((lefts, rows), 0) == SECOND + PART

    def turn(g, carry):
        t0 = pl.multiple_of(g * GROUP, GROUP)
        here = pl.ds(t0, GROUP)
        slabs = [
            own[:PART, here, :],
            own[PART : PART + 7, here, :],
            own[PART:, here, :],
            wres_vm[here, :].reshape(1, GROUP, rows),
            own[PART + 7 : PART + 13, here, :],
            own[PART + 13 :, here, :],
            jnp.zeros((4, GROUP, rows), BF16),
        ]
        turned = pltpu.einshape("ktr->tkr", jnp.concatenate(slabs, axis=0))
        group_weight = weight_vm[here, :]
        for u in range(GROUP):
            left = turned[u][:lefts]
            scaled = (left.astype(F32) * group_weight[u : u + 1, :]).astype(BF16)
            scaled = jnp.where(is_wres, left, scaled)
            left_out[t0 + u] = scaled
            out = dot(scaled, turned[u], ((1,), (1,)))
            value = jnp.where(kept, jnp.where(second, out[SECOND:], out[:SECOND]), 0.0)
            base = base_row(pulsar_sm[0, t0 + u], near, message, head)
            acc[pl.ds(base, WIDE), :wide] += value[:WIDE]
        return carry

    lax.fori_loop(0, tiles // GROUP, turn, 0)


def cross_kernel(near, far, pulsar_sm, left, acc_own, other, out, acc):
    cols, tiles, rows = other.shape
    head = 2 * far
    message = head + far * WIDE
    core = lax.axis_index("rep")
    acc[...] = jnp.zeros_like(acc)
    second = iota((SECOND, cols), 1) >= PART

    def turn(g, carry):
        t0 = pl.multiple_of(g * GROUP, GROUP)
        here = pl.ds(t0, GROUP)
        slabs = [other[pl.ds(PART * core, PART), here, :], other[pl.ds(PART - PART * core, PART), here, :]]
        turned = pltpu.einshape("ktr->tkr", jnp.concatenate(slabs, axis=0))
        for u in range(GROUP):
            product = dot(left[t0 + u], turned[u], ((1,), (1,)))
            value = jnp.where(second, product[SECOND:], product[:SECOND])
            base = base_row(pulsar_sm[0, t0 + u], near, message, head)
            acc[pl.ds(base, PART), :cols] += value[:PART]
        return carry

    lax.fori_loop(0, tiles // GROUP, turn, 0)

    lane, row = iota((message, LANES), 1), iota((message, LANES), 0) - head
    rest_here = (row >= 0) & (row % WIDE == PART) & (lane >= LANES // 2)

    def pack(n, carry):
        here = pl.ds(pl.multiple_of(n * message, 8), message)
        value = acc_own[here, :] + pltpu.roll(acc[here, :], CROSS, 1)
        rest = pltpu.roll(value - value.astype(BF16).astype(F32), LANES // 2, 1)
        out[n] = jnp.where(rest_here, rest, value).astype(BF16)
        return carry

    lax.fori_loop(0, near, pack, 0)


def near_kernel(far, got, out, total):
    near = got.shape[0]
    head = 2 * far
    for half in range(2):
        part = got[:, half * far : (half + 1) * far, :].astype(F32)
        out[:, half * near : (half + 1) * near, :] = jnp.swapaxes(part, 0, 1).astype(BF16)
    summed = got[0, head:, :].astype(F32)
    for n in range(1, near):
        summed = summed + got[n, head:, :].astype(F32)
    total[: far * WIDE, :] = summed
    total[far * WIDE :, :] = jnp.zeros((total.shape[0] - far * WIDE, LANES), F32)
    lane, row = iota((SECOND, LANES), 1), iota((SECOND, LANES), 0)
    for f in range(far):
        block = total[f * WIDE : f * WIDE + SECOND, :]
        joined = block + pltpu.roll(block, LANES // 2, 1)
        rest = joined - joined.astype(BF16).astype(F32)
        split = jnp.where(lane < LANES // 2, joined, rest)
        out[f, WHITE:, :] = jnp.where(row == PART, split, block).astype(BF16)


def far_kernel(got, out):
    total = got[0, WHITE:, :].astype(F32)
    for f in range(1, got.shape[0]):
        total = total + got[f, WHITE:, :].astype(F32)
    out[...] = total


def white_kernel(got, white):
    far, near = got.shape[0], WHITE // 2
    tiles = far * near
    lane = iota((near, LANES), 1)
    puts = []
    for f in range(far):
        value = got[f, WHITE : WHITE + near, :].astype(F32)
        place = jnp.sum(jnp.where(lane == PLACE, value, 0.0), axis=1, keepdims=True)
        puts.append((lane.astype(F32) == place).astype(F32))
    put = jnp.concatenate(puts, axis=0).astype(BF16)
    for half in range(2):
        rows = got[:, half * near : (half + 1) * near, :].reshape(tiles, LANES)
        white[:, half * LANES : (half + 1) * LANES] = dot(put, rows, ((0,), (0,)))


def join_kernel(mine_in, theirs_in, gram, proj):
    mine, theirs = mine_in[...], theirs_in[...]
    lane = iota((SECOND, LANES), 1)

    def square(a):
        return jnp.concatenate([a, jnp.zeros((LANES - SECOND, LANES), F32)], axis=0).T

    cross = pltpu.roll(mine, LANES - CROSS, 1)
    turned = square(mine)[SECOND : 2 * SECOND]
    theirs_t = square(pltpu.roll(theirs, LANES - CROSS, 1))
    theirs_0 = theirs_t[:SECOND]
    theirs_1 = theirs_t[PART : PART + SECOND]

    def laid(pieces):
        value = jnp.zeros((SECOND, LANES), F32)
        for source, start, width, to in pieces:
            moved = pltpu.roll(source, (to - start) % LANES, 1) if to != start else source
            value = jnp.where((lane >= to) & (lane < to + width), moved, value)
        return value

    def write(own, cross_at):
        low, high = cross_at
        top = [(mine, 0, PART, own), (mine, SECOND, PART, own + PART)]
        under = [(turned, 0, PART, own)]
        under += [(mine, at, b - a, own + PART + a) for a, b, at in DIAGONAL]
        if own == 0:
            top += [(cross, 0, PART, low), (theirs_1, 0, PART, high)]
            under += [(theirs_0, 0, PART, low), (cross, PART, PART, high)]
        else:
            top += [(theirs_0, 0, PART, low), (cross, 0, PART, high)]
            under += [(cross, PART, PART, low), (theirs_1, 0, PART, high)]
        gram[:PART, :] = laid(top)[:PART, : 4 * PART]
        gram[PART:, :] = laid(under)[:PART, : 4 * PART]

    core = lax.axis_index("rep")

    @pl.when(core == 0)
    def _():
        write(0, (2 * PART, 3 * PART))

    @pl.when(core == 1)
    def _():
        write(2 * PART, (0, PART))

    sums = mine + pltpu.roll(mine, LANES // 2, 1)
    proj[...] = laid([(sums, 0, PART, 0), (sums, SECOND, PART, PART)])[PART:WIDE, : 2 * PART]


def vmem(n):
    return [pl.BlockSpec(memory_space=pltpu.VMEM)] * n


SMEM = pl.BlockSpec(memory_space=pltpu.SMEM)
ANY = pl.BlockSpec(memory_space=pl.ANY)
SWAP = [(0, 1), (1, 0)]


def shards(
    residual, toa_error, basis_rows, efac_table, equad_table, pulsar, backend, counts, owner_slot
):
    far, near = lax.axis_size(FAR), lax.axis_size(NEAR)
    tiles, cols, rows = basis_rows.shape
    own = jnp.transpose(basis_rows, (1, 0, 2))
    other = lax.ppermute(own, "rep", SWAP)
    message = 2 * far + far * WIDE
    line = lambda a: a.reshape(1, -1)
    ints = [line(a) for a in (pulsar, backend, counts, owner_slot)]
    left, acc = pl.pallas_call(
        functools.partial(own_kernel, near, far),
        out_shape=(
            jax.ShapeDtypeStruct((tiles, 2 * SECOND, rows), BF16),
            jax.ShapeDtypeStruct((near * message, LANES), F32),
        ),
        in_specs=[ANY] * 9,
        out_specs=tuple(vmem(2)),
        scratch_shapes=[pltpu.VMEM((1, tiles), jnp.int32)] * 4
        + [pltpu.VMEM((tiles, rows), F32)] * 2
        + [pltpu.VMEM(efac_table.shape[::-1], F32)] * 2
        + [
            pltpu.VMEM(own.shape, BF16),
            pltpu.SMEM((1, tiles), jnp.int32),
            pltpu.VMEM((tiles, rows), F32),
            pltpu.VMEM((tiles, rows), BF16),
            pltpu.SemaphoreType.DMA((10,)),
        ],
        compiler_params=pltpu.CompilerParams(vmem_limit_bytes=32 << 20),
        cost_estimate=pl.CostEstimate(flops=2 * 10**9, transcendentals=0, bytes_accessed=10**7),
        name="own",
    )(*ints, residual, toa_error, efac_table.T, equad_table.T, own)
    sent = pl.pallas_call(
        functools.partial(cross_kernel, near, far),
        out_shape=jax.ShapeDtypeStruct((near, message, LANES), BF16),
        in_specs=[SMEM] + vmem(3),
        out_specs=vmem(1)[0],
        scratch_shapes=[pltpu.VMEM((near * message, LANES), F32)],
        compiler_params=pltpu.CompilerParams(vmem_limit_bytes=32 << 20),
        name="cross",
    )(ints[0], left, acc, other)
    got = lax.all_to_all(sent, NEAR, 0, 0, tiled=True)
    sent = pl.pallas_call(
        functools.partial(near_kernel, far),
        out_shape=jax.ShapeDtypeStruct((far, WHITE + SECOND, LANES), BF16),
        in_specs=vmem(1),
        out_specs=vmem(1)[0],
        scratch_shapes=[pltpu.VMEM((far * WIDE + 8, LANES), F32)],
        name="near_sum",
    )(got)
    got = lax.all_to_all(sent, FAR, 0, 0, tiled=True)
    mine = pl.pallas_call(
        far_kernel,
        out_shape=jax.ShapeDtypeStruct((SECOND, LANES), F32),
        in_specs=vmem(1),
        out_specs=vmem(1)[0],
        name="far_sum",
    )(got)
    theirs = lax.ppermute(mine, "rep", SWAP)
    whitened = pl.pallas_call(
        white_kernel,
        out_shape=jax.ShapeDtypeStruct((tiles, rows), F32),
        in_specs=vmem(1),
        out_specs=vmem(1)[0],
        cost_estimate=pl.CostEstimate(flops=10**7, transcendentals=0, bytes_accessed=10**6),
        name="white",
    )(got)
    gram, projection = pl.pallas_call(
        join_kernel,
        out_shape=(
            jax.ShapeDtypeStruct((cols, 2 * cols), F32),
            jax.ShapeDtypeStruct((1, cols), F32),
        ),
        in_specs=vmem(2),
        out_specs=tuple(vmem(2)),
        name="join",
    )(mine, theirs)
    return gram.T[None], projection, whitened


def solution(mesh):
    split = Mesh(
        mesh.devices.reshape(8, 4, 4, mesh.shape["rep"]), ("toa_0", "toa_1", "toa_2", "rep")
    )
    placed = (
        P(TOA, None),
        P(TOA, None),
        P(TOA, "rep", None),
        P(),
        P(),
        P(TOA),
        P(TOA),
        P(TOA),
        P(TOA),
    )
    return jax.shard_map(
        shards,
        mesh=split,
        in_specs=placed,
        out_specs=(P(TOA, None, "rep"), P(TOA, "rep"), P(TOA, None)),
        check_vma=False,
    )
```

```python
import functools

import jax
import jax.numpy as jnp
from jax import lax
from jax.experimental import pallas as pl
from jax.experimental.pallas import tpu as pltpu
from jax.sharding import Mesh
from jax.sharding import PartitionSpec as P

TOA = ("toa_0", "toa_1", "toa_2")
FAR, NEAR = "toa_0", ("toa_1", "toa_2")
BF16, F32 = jnp.bfloat16, jnp.float32
LANES = 128
GROUP = 16

PART = 25
WIDE = PART + 1
SECOND = 32
DIAGONAL = ((0, 7, 25), (7, 13, 58), (13, 25, 64))
CROSS = 76
PLACE = 126
WHITE = 32


def dot(a, b, dims=((1,), (0,)), **kw):
    return lax.dot_general(a, b, (dims, ((), ())), preferred_element_type=F32, **kw)


def iota(shape, dim):
    return lax.broadcasted_iota(jnp.int32, shape, dim)


def as_column(row, lanes):
    square = jnp.broadcast_to(row, (LANES, row.shape[1])).T
    return jnp.concatenate([square] * (lanes // LANES), axis=1)


def base_row(p, near, message, head):
    return (p % near) * message + head + (p // near) * WIDE


def own_kernel(
    near, far, pulsar_in, backend_in, counts_in, slot_in, residual_in, error_in, efac_in, equad_in,
    own_in, left_out, acc,
    pulsar, backend, counts, slot, residual, error, efac_t, equad_t, own, pulsar_sm,
    weight_vm, wres_vm, sems,
):
    cols, tiles, rows = own.shape
    head = 2 * far
    message = head + far * WIDE
    pulsars, backends = efac_t.shape[1], efac_t.shape[0]
    pairs = (
        (pulsar_in, pulsar), (backend_in, backend), (counts_in, counts), (slot_in, slot),
        (residual_in, residual), (error_in, error), (efac_in, efac_t), (equad_in, equad_t),
        (pulsar_in, pulsar_sm), (own_in, own),
    )
    copies = [pltpu.make_async_copy(a, b, sems.at[i]) for i, (a, b) in enumerate(pairs)]
    for copy in copies:
        copy.start()
    acc[...] = jnp.zeros_like(acc)
    for copy in copies[:-1]:
        copy.wait()

    of_pulsar = (iota((pulsars, tiles), 0) == pulsar[...]).astype(F32)
    of_backend = (iota((backends, tiles), 0) == backend[...]).astype(F32)
    high = dict(precision=lax.Precision.HIGHEST)
    factor = jnp.sum(dot(efac_t[...], of_pulsar, **high) * of_backend, axis=0, keepdims=True)
    floor = jnp.sum(dot(equad_t[...], of_pulsar, **high) * of_backend, axis=0, keepdims=True)
    factor2 = as_column(factor * factor, rows)
    floor2 = as_column(floor * floor, rows)
    count = as_column(counts[...].astype(F32), rows)
    valid = iota((tiles, rows), 1).astype(F32) < count
    weight = jnp.where(valid, 1.0 / (factor2 * error[...] ** 2 + floor2), 0.0)
    weight_vm[...] = weight
    wres_vm[...] = (weight * residual[...]).astype(BF16)
    white = (jnp.sqrt(weight) * residual[...]).astype(BF16)

    me = lax.axis_index("toa_1") * lax.axis_size("toa_2") + lax.axis_index("toa_2")
    dest = slot[...] // tiles
    place = (slot[...] % tiles).astype(F32)
    order = (dest % near) * far + dest // near
    moved = (iota((tiles, tiles), 0) == order).astype(BF16)
    white_to = dot(moved, white)
    place_to = dot(moved, as_column(place, LANES).astype(BF16))
    place_to = jnp.where(iota(place_to.shape, 1) == PLACE, place_to, 0.0)
    for n in range(near):
        at = n * message
        acc[at : at + far, :] = white_to[n * far : (n + 1) * far, :LANES]
        acc[at + far : at + 2 * far, :] = white_to[n * far : (n + 1) * far, LANES:]
        acc[pl.ds(at + head + me, far, stride=WIDE), :] = place_to[n * far : (n + 1) * far, :]
    copies[-1].wait()

    lefts = 2 * SECOND
    wide = 80
    lane, row = iota((SECOND, wide), 1), iota((SECOND, wide), 0)
    own_lane = (lane < PART) | ((lane >= SECOND) & (lane < SECOND + PART))
    second = (~own_lane) | (row == PART)
    kept = own_lane | (row != PART)
    is_wres = iota((lefts, rows), 0) == SECOND + PART

    def turn(g, carry):
        t0 = pl.multiple_of(g * GROUP, GROUP)
        here = pl.ds(t0, GROUP)
        slabs = [
            own[:PART, here, :],
            own[PART : PART + 7, here, :],
            own[PART:, here, :],
            wres_vm[here, :].reshape(1, GROUP, rows),
            own[PART + 7 : PART + 13, here, :],
            own[PART + 13 :, here, :],
            jnp.zeros((4, GROUP, rows), BF16),
        ]
        turned = pltpu.einshape("ktr->tkr", jnp.concatenate(slabs, axis=0))
        group_weight = weight_vm[here, :]
        for u in range(GROUP):
            left = turned[u][:lefts]
            scaled = (left.astype(F32) * group_weight[u : u + 1, :]).astype(BF16)
            scaled = jnp.where(is_wres, left, scaled)
            left_out[t0 + u] = scaled
            out = dot(scaled, turned[u], ((1,), (1,)))
            value = jnp.where(kept, jnp.where(second, out[SECOND:], out[:SECOND]), 0.0)
            base = base_row(pulsar_sm[0, t0 + u], near, message, head)
            acc[pl.ds(base, WIDE), :wide] += value[:WIDE]
        return carry

    lax.fori_loop(0, tiles // GROUP, turn, 0)


def cross_kernel(near, far, pulsar_sm, left, acc_own, other, out, acc):
    cols, tiles, rows = other.shape
    head = 2 * far
    message = head + far * WIDE
    core = lax.axis_index("rep")
    acc[...] = jnp.zeros_like(acc)
    second = iota((SECOND, cols), 1) >= PART

    def turn(g, carry):
        t0 = pl.multiple_of(g * GROUP, GROUP)
        here = pl.ds(t0, GROUP)
        slabs = [other[pl.ds(PART * core, PART), here, :], other[pl.ds(PART - PART * core, PART), here, :]]
        turned = pltpu.einshape("ktr->tkr", jnp.concatenate(slabs, axis=0))
        for u in range(GROUP):
            product = dot(left[t0 + u], turned[u], ((1,), (1,)))
            value = jnp.where(second, product[SECOND:], product[:SECOND])
            base = base_row(pulsar_sm[0, t0 + u], near, message, head)
            acc[pl.ds(base, PART), :cols] += value[:PART]
        return carry

    lax.fori_loop(0, tiles // GROUP, turn, 0)

    lane, row = iota((message, LANES), 1), iota((message, LANES), 0) - head
    rest_here = (row >= 0) & (row % WIDE == PART) & (lane >= LANES // 2)

    def pack(n, carry):
        here = pl.ds(pl.multiple_of(n * message, 8), message)
        value = acc_own[here, :] + pltpu.roll(acc[here, :], CROSS, 1)
        rest = pltpu.roll(value - value.astype(BF16).astype(F32), LANES // 2, 1)
        out[n] = jnp.where(rest_here, rest, value).astype(BF16)
        return carry

    lax.fori_loop(0, near, pack, 0)


def near_kernel(far, got, out, total):
    near = got.shape[0]
    head = 2 * far
    for half in range(2):
        part = got[:, half * far : (half + 1) * far, :].astype(F32)
        out[:, half * near : (half + 1) * near, :] = jnp.swapaxes(part, 0, 1).astype(BF16)
    summed = got[0, head:, :].astype(F32)
    for n in range(1, near):
        summed = summed + got[n, head:, :].astype(F32)
    total[: far * WIDE, :] = summed
    total[far * WIDE :, :] = jnp.zeros((total.shape[0] - far * WIDE, LANES), F32)
    lane, row = iota((SECOND, LANES), 1), iota((SECOND, LANES), 0)
    for f in range(far):
        block = total[f * WIDE : f * WIDE + SECOND, :]
        joined = block + pltpu.roll(block, LANES // 2, 1)
        rest = joined - joined.astype(BF16).astype(F32)
        split = jnp.where(lane < LANES // 2, joined, rest)
        out[f, WHITE:, :] = jnp.where(row == PART, split, block).astype(BF16)


def far_kernel(got, out):
    total = got[0, WHITE:, :].astype(F32)
    for f in range(1, got.shape[0]):
        total = total + got[f, WHITE:, :].astype(F32)
    out[...] = total


def white_kernel(got, white):
    far, near = got.shape[0], WHITE // 2
    tiles = far * near
    lane = iota((near, LANES), 1)
    puts = []
    for f in range(far):
        value = got[f, WHITE : WHITE + near, :].astype(F32)
        place = jnp.sum(jnp.where(lane == PLACE, value, 0.0), axis=1, keepdims=True)
        puts.append((lane.astype(F32) == place).astype(F32))
    put = jnp.concatenate(puts, axis=0).astype(BF16)
    for half in range(2):
        rows = got[:, half * near : (half + 1) * near, :].reshape(tiles, LANES)
        white[:, half * LANES : (half + 1) * LANES] = dot(put, rows, ((0,), (0,)))


def join_kernel(mine_in, theirs_in, gram, proj):
    mine, theirs = mine_in[...], theirs_in[...]
    lane = iota((SECOND, LANES), 1)

    def square(a):
        return jnp.concatenate([a, jnp.zeros((LANES - SECOND, LANES), F32)], axis=0).T

    cross = pltpu.roll(mine, LANES - CROSS, 1)
    turned = square(mine)[SECOND : 2 * SECOND]
    theirs_t = square(pltpu.roll(theirs, LANES - CROSS, 1))
    theirs_0 = theirs_t[:SECOND]
    theirs_1 = theirs_t[PART : PART + SECOND]

    def laid(pieces):
        value = jnp.zeros((SECOND, LANES), F32)
        for source, start, width, to in pieces:
            moved = pltpu.roll(source, (to - start) % LANES, 1) if to != start else source
            value = jnp.where((lane >= to) & (lane < to + width), moved, value)
        return value

    def write(own, cross_at):
        low, high = cross_at
        top = [(mine, 0, PART, own), (mine, SECOND, PART, own + PART)]
        under = [(turned, 0, PART, own)]
        under += [(mine, at, b - a, own + PART + a) for a, b, at in DIAGONAL]
        if own == 0:
            top += [(cross, 0, PART, low), (theirs_1, 0, PART, high)]
            under += [(theirs_0, 0, PART, low), (cross, PART, PART, high)]
        else:
            top += [(theirs_0, 0, PART, low), (cross, 0, PART, high)]
            under += [(cross, PART, PART, low), (theirs_1, 0, PART, high)]
        gram[:PART, 0, :] = laid(top)[:PART, : 4 * PART]
        gram[PART:, 0, :] = laid(under)[:PART, : 4 * PART]

    core = lax.axis_index("rep")

    @pl.when(core == 0)
    def _():
        write(0, (2 * PART, 3 * PART))

    @pl.when(core == 1)
    def _():
        write(2 * PART, (0, PART))

    sums = mine + pltpu.roll(mine, LANES // 2, 1)
    proj[...] = laid([(sums, 0, PART, 0), (sums, SECOND, PART, PART)])[PART:WIDE, : 2 * PART]


def vmem(n):
    return [pl.BlockSpec(memory_space=pltpu.VMEM)] * n


SMEM = pl.BlockSpec(memory_space=pltpu.SMEM)
HBM = pl.BlockSpec(memory_space=pltpu.HBM)
SWAP = [(0, 1), (1, 0)]


def stay(a):
    return pltpu.with_memory_space_constraint(a, pltpu.HBM)


def near_by(a):
    return pltpu.with_memory_space_constraint(a, pltpu.VMEM)


def shards(
    residual, toa_error, basis_rows, efac_table, equad_table, pulsar, backend, counts, owner_slot
):
    far, near = lax.axis_size(FAR), lax.axis_size(NEAR)
    tiles, cols, rows = basis_rows.shape
    own = jnp.transpose(basis_rows, (1, 0, 2))
    other = lax.ppermute(own, "rep", SWAP)
    message = 2 * far + far * WIDE
    line = lambda a: a.reshape(1, -1)
    ints = [line(a) for a in (pulsar, backend, counts, owner_slot)]
    left, acc = pl.pallas_call(
        functools.partial(own_kernel, near, far),
        out_shape=(
            jax.ShapeDtypeStruct((tiles, 2 * SECOND, rows), BF16),
            jax.ShapeDtypeStruct((near * message, LANES), F32),
        ),
        in_specs=[HBM] * 9,
        out_specs=tuple(vmem(2)),
        scratch_shapes=[pltpu.VMEM((1, tiles), jnp.int32)] * 4
        + [pltpu.VMEM((tiles, rows), F32)] * 2
        + [pltpu.VMEM(efac_table.shape[::-1], F32)] * 2
        + [
            pltpu.VMEM(own.shape, BF16),
            pltpu.SMEM((1, tiles), jnp.int32),
            pltpu.VMEM((tiles, rows), F32),
            pltpu.VMEM((tiles, rows), BF16),
            pltpu.SemaphoreType.DMA((10,)),
        ],
        compiler_params=pltpu.CompilerParams(vmem_limit_bytes=32 << 20),
        cost_estimate=pl.CostEstimate(flops=2 * 10**9, transcendentals=0, bytes_accessed=10**7),
        name="own",
    )(*map(stay, (*ints, residual, toa_error, efac_table.T, equad_table.T, own)))
    sent = pl.pallas_call(
        functools.partial(cross_kernel, near, far),
        out_shape=jax.ShapeDtypeStruct((near, message, LANES), BF16),
        in_specs=[SMEM] + vmem(3),
        out_specs=vmem(1)[0],
        scratch_shapes=[pltpu.VMEM((near * message, LANES), F32)],
        compiler_params=pltpu.CompilerParams(vmem_limit_bytes=32 << 20),
        name="cross",
    )(ints[0], left, acc, other)
    got = lax.all_to_all(sent, NEAR, 0, 0, tiled=True)
    sent = pl.pallas_call(
        functools.partial(near_kernel, far),
        out_shape=pltpu.VMEM((far, WHITE + SECOND, LANES), BF16),
        in_specs=vmem(1),
        out_specs=vmem(1)[0],
        scratch_shapes=[pltpu.VMEM((far * WIDE + 8, LANES), F32)],
        name="near_sum",
    )(near_by(got))
    got = lax.all_to_all(sent, FAR, 0, 0, tiled=True)
    mine = pl.pallas_call(
        far_kernel,
        out_shape=pltpu.VMEM((SECOND, LANES), F32),
        in_specs=vmem(1),
        out_specs=vmem(1)[0],
        name="far_sum",
    )(near_by(got))
    theirs = lax.ppermute(mine, "rep", SWAP)
    whitened = pl.pallas_call(
        white_kernel,
        out_shape=jax.ShapeDtypeStruct((tiles, rows), F32),
        in_specs=vmem(1),
        out_specs=vmem(1)[0],
        cost_estimate=pl.CostEstimate(flops=10**7, transcendentals=0, bytes_accessed=10**6),
        name="white",
    )(near_by(got))
    gram, projection = pl.pallas_call(
        join_kernel,
        out_shape=(
            jax.ShapeDtypeStruct((cols, 1, 2 * cols), F32),
            jax.ShapeDtypeStruct((1, cols), F32),
        ),
        in_specs=vmem(2),
        out_specs=tuple(vmem(2)),
        name="join",
    )(near_by(mine), near_by(theirs))
    return jnp.transpose(gram, (1, 2, 0)), projection, whitened


def solution(mesh):
    split = Mesh(
        mesh.devices.reshape(8, 4, 4, mesh.shape["rep"]), ("toa_0", "toa_1", "toa_2", "rep")
    )
    placed = (
        P(TOA, None),
        P(TOA, None),
        P(TOA, "rep", None),
        P(),
        P(),
        P(TOA),
        P(TOA),
        P(TOA),
        P(TOA),
    )
    return jax.shard_map(
        shards,
        mesh=split,
        in_specs=placed,
        out_specs=(P(TOA, None, "rep"), P(TOA, "rep"), P(TOA, None)),
        check_vma=False,
    )
```

```python
import functools

import jax
import jax.numpy as jnp
from jax import lax
from jax.experimental import pallas as pl
from jax.experimental.pallas import tpu as pltpu
from jax.sharding import Mesh
from jax.sharding import PartitionSpec as P

TOA = ("toa_0", "toa_1", "toa_2")
FAR, NEAR = "toa_0", ("toa_1", "toa_2")
BF16, F32 = jnp.bfloat16, jnp.float32
LANES = 128
GROUP = 16

PART = 25
WIDE = PART + 1
SECOND = 32
OWN = 2 * PART
OWN2 = OWN + SECOND
DIAGONAL = ((0, 7, 75), (7, 13, 108), (13, 25, 114))
PLACE = 126
WHITE = 16


def dot(a, b, dims=((1,), (0,)), **kw):
    return lax.dot_general(a, b, (dims, ((), ())), preferred_element_type=F32, **kw)


def iota(shape, dim):
    return lax.broadcasted_iota(jnp.int32, shape, dim)


def as_column(row, lanes):
    square = jnp.broadcast_to(row, (LANES, row.shape[1])).T
    return jnp.concatenate([square] * (lanes // LANES), axis=1)


def base_row(p, near, message, head):
    return (p % near) * message + head + (p // near) * WIDE


def value_lanes(shape):
    lane = iota(shape, 1)
    return ((lane >= OWN) & (lane < OWN + PART)) | ((lane >= OWN2) & (lane < OWN2 + PART))


def split(value):
    here = value_lanes(value.shape)
    rest = jnp.where(here, value - value.astype(BF16).astype(F32), 0.0)
    return jnp.where(here, value, pltpu.roll(rest, LANES // 2, 1))


def own_kernel(
    near, far, pulsar_in, backend_in, counts_in, slot_in, residual_in, error_in, efac_in, equad_in,
    own_in, left_out, acc,
    pulsar, backend, counts, slot, residual, error, efac_t, equad_t, own, pulsar_sm,
    weight_vm, wres_vm, sems, own_sems,
):
    cols, tiles, rows = own.shape
    message = far + far * WIDE
    pulsars, backends = efac_t.shape[1], efac_t.shape[0]
    pairs = (
        (pulsar_in, pulsar), (backend_in, backend), (counts_in, counts), (slot_in, slot),
        (residual_in, residual), (error_in, error), (efac_in, efac_t), (equad_in, equad_t),
        (pulsar_in, pulsar_sm),
    )
    copies = [pltpu.make_async_copy(a, b, sems.at[i]) for i, (a, b) in enumerate(pairs)]

    def own_copy(g):
        here = pl.ds(pl.multiple_of(g * GROUP, GROUP), GROUP)
        return pltpu.make_async_copy(own_in.at[:, here, :], own.at[:, here, :], own_sems.at[g])

    for copy in copies:
        copy.start()
    for g in range(tiles // GROUP):
        own_copy(g).start()
    acc[...] = jnp.zeros_like(acc)
    for copy in copies:
        copy.wait()

    of_pulsar = (iota((pulsars, tiles), 0) == pulsar[...]).astype(F32)
    of_backend = (iota((backends, tiles), 0) == backend[...]).astype(F32)
    high = dict(precision=lax.Precision.HIGHEST)
    factor = jnp.sum(dot(efac_t[...], of_pulsar, **high) * of_backend, axis=0, keepdims=True)
    floor = jnp.sum(dot(equad_t[...], of_pulsar, **high) * of_backend, axis=0, keepdims=True)
    factor2 = as_column(factor * factor, rows)
    floor2 = as_column(floor * floor, rows)
    count = as_column(counts[...].astype(F32), rows)
    valid = iota((tiles, rows), 1).astype(F32) < count
    weight = jnp.where(valid, 1.0 / (factor2 * error[...] ** 2 + floor2), 0.0)
    weight_vm[...] = weight
    wres_vm[...] = (weight * residual[...]).astype(BF16)
    white = jnp.sqrt(weight) * residual[...]
    white = jnp.where(lax.axis_index("rep") == 0, white[:, :LANES], white[:, LANES:])

    me = lax.axis_index("toa_1") * lax.axis_size("toa_2") + lax.axis_index("toa_2")
    dest = slot[...] // tiles
    place = (slot[...] % tiles).astype(F32)
    order = (dest % near) * far + dest // near
    moved = (iota((tiles, tiles), 0) == order).astype(BF16)
    white_to = dot(moved, white.astype(BF16))
    place_to = dot(moved, as_column(place, LANES).astype(BF16))
    place_to = jnp.where(iota(place_to.shape, 1) == PLACE, place_to, 0.0)
    for n in range(near):
        at = n * message
        acc[at : at + far, :] = white_to[n * far : (n + 1) * far, :]
        acc[pl.ds(at + far + me, far, stride=WIDE), :] = place_to[n * far : (n + 1) * far, :]

    lefts = 2 * SECOND
    wide = 80
    lane, row = iota((SECOND, wide), 1), iota((SECOND, wide), 0)
    own_lane = (lane < PART) | ((lane >= SECOND) & (lane < SECOND + PART))
    second = (~own_lane) | (row == PART)
    kept = own_lane | (row != PART)
    is_wres = iota((lefts, rows), 0) == SECOND + PART

    def turn(g, carry):
        t0 = pl.multiple_of(g * GROUP, GROUP)
        here = pl.ds(t0, GROUP)
        own_copy(g).wait()
        slabs = [
            own[:PART, here, :],
            own[PART : PART + 7, here, :],
            own[PART:, here, :],
            wres_vm[here, :].reshape(1, GROUP, rows),
            own[PART + 7 : PART + 13, here, :],
            own[PART + 13 :, here, :],
            jnp.zeros((4, GROUP, rows), BF16),
        ]
        turned = pltpu.einshape("ktr->tkr", jnp.concatenate(slabs, axis=0))
        group_weight = weight_vm[here, :]
        for u in range(GROUP):
            left = turned[u][:lefts]
            scaled = (left.astype(F32) * group_weight[u : u + 1, :]).astype(BF16)
            scaled = jnp.where(is_wres, left, scaled)
            left_out[t0 + u] = scaled
            out = dot(scaled, turned[u], ((1,), (1,)))
            value = jnp.where(kept, jnp.where(second, out[SECOND:], out[:SECOND]), 0.0)
            base = base_row(pulsar_sm[0, t0 + u], near, message, far)
            acc[pl.ds(base, WIDE), OWN : OWN + wide - 4] += value[:WIDE, : wide - 4]
        return carry

    lax.fori_loop(0, tiles // GROUP, turn, 0)
    for n in range(near):
        here = pl.ds(n * message + far + PART, far, stride=WIDE)
        acc[here, :] = split(acc[here, :])


def cross_kernel(near, far, pulsar_sm, left, acc_in, other, out, acc):
    cols, tiles, rows = other.shape
    message = far + far * WIDE
    core = lax.axis_index("rep")
    second = iota((SECOND, cols), 1) >= PART

    def turn(g, carry):
        t0 = pl.multiple_of(g * GROUP, GROUP)
        here = pl.ds(t0, GROUP)
        slabs = [other[pl.ds(PART * core, PART), here, :], other[pl.ds(PART - PART * core, PART), here, :]]
        turned = pltpu.einshape("ktr->tkr", jnp.concatenate(slabs, axis=0))
        for u in range(GROUP):
            product = dot(left[t0 + u], turned[u], ((1,), (1,)))
            value = jnp.where(second, product[SECOND:], product[:SECOND])
            base = base_row(pulsar_sm[0, t0 + u], near, message, far)
            acc[pl.ds(base, PART), :cols] += value[:PART]
        return carry

    lax.fori_loop(0, tiles // GROUP, turn, 0)

    def pack(n, carry):
        out[n] = acc[pl.ds(pl.multiple_of(n * message, 8), message), :].astype(BF16)
        return carry

    lax.fori_loop(0, near, pack, 0)


def near_kernel(far, got, out, total):
    near = got.shape[0]
    part = got[:, :far, :].astype(F32)
    out[:, :near, :] = jnp.swapaxes(part, 0, 1).astype(BF16)
    summed = got[0, far:, :].astype(F32)
    for n in range(1, near):
        summed = summed + got[n, far:, :].astype(F32)
    total[: far * WIDE, :] = summed
    total[far * WIDE :, :] = jnp.zeros((total.shape[0] - far * WIDE, LANES), F32)
    row = iota((SECOND, LANES), 0)
    for f in range(far):
        block = total[f * WIDE : f * WIDE + SECOND, :]
        whole = split(block + pltpu.roll(block, LANES // 2, 1))
        out[f, WHITE:, :] = jnp.where(row == PART, whole, block).astype(BF16)


def far_kernel(got, out):
    far, near = got.shape[0], WHITE
    tiles = far * near
    total = got[0, WHITE:, :].astype(F32)
    for f in range(1, far):
        total = total + got[f, WHITE:, :].astype(F32)
    out[:SECOND, :] = total
    lane = iota((near, LANES), 1)
    puts = []
    for f in range(far):
        value = got[f, WHITE : WHITE + near, :].astype(F32)
        place = jnp.sum(jnp.where(lane == PLACE, value, 0.0), axis=1, keepdims=True)
        puts.append((lane.astype(F32) == place).astype(F32))
    put = jnp.concatenate(puts, axis=0).astype(BF16)
    out[SECOND:, :] = dot(put, got[:, :near, :].reshape(tiles, LANES), ((0,), (0,)))


def join_kernel(mine_in, theirs_in, gram, proj, white):
    mine, theirs = mine_in[:SECOND, :], theirs_in[:SECOND, :]
    lane = iota((SECOND, LANES), 1)

    def square(a):
        return jnp.concatenate([a, jnp.zeros((LANES - SECOND, LANES), F32)], axis=0).T

    turned = square(pltpu.roll(mine, LANES - OWN2, 1))[:SECOND]
    theirs_t = square(theirs)
    theirs_0 = theirs_t[:SECOND]
    theirs_1 = theirs_t[PART : PART + SECOND]

    def laid(pieces):
        value = jnp.zeros((SECOND, LANES), F32)
        for source, start, width, to in pieces:
            moved = pltpu.roll(source, (to - start) % LANES, 1) if to != start else source
            value = jnp.where((lane >= to) & (lane < to + width), moved, value)
        return value

    def write(own, low, high):
        top = [(mine, OWN, PART, own), (mine, OWN2, PART, own + PART)]
        under = [(turned, 0, PART, own)]
        under += [(mine, at, b - a, own + PART + a) for a, b, at in DIAGONAL]
        if own == 0:
            top += [(mine, 0, PART, low), (theirs_1, 0, PART, high)]
            under += [(theirs_0, 0, PART, low), (mine, PART, PART, high)]
        else:
            top += [(theirs_0, 0, PART, low), (mine, 0, PART, high)]
            under += [(mine, PART, PART, low), (theirs_1, 0, PART, high)]
        gram[:PART, 0, :] = laid(top)[:PART, : 4 * PART]
        gram[PART:, 0, :] = laid(under)[:PART, : 4 * PART]
        halves = (mine_in, theirs_in) if own == 0 else (theirs_in, mine_in)
        for i, half in enumerate(halves):
            white[:, i * LANES : (i + 1) * LANES] = half[SECOND:, :]

    core = lax.axis_index("rep")

    @pl.when(core == 0)
    def _():
        write(0, 2 * PART, 3 * PART)

    @pl.when(core == 1)
    def _():
        write(2 * PART, 0, PART)

    sums = mine + pltpu.roll(mine, LANES // 2, 1)
    proj[...] = laid([(sums, OWN, PART, 0), (sums, OWN2, PART, PART)])[PART:WIDE, : 2 * PART]


def vmem(n):
    return [pl.BlockSpec(memory_space=pltpu.VMEM)] * n


SMEM = pl.BlockSpec(memory_space=pltpu.SMEM)
HBM = pl.BlockSpec(memory_space=pltpu.HBM)
SWAP = [(0, 1), (1, 0)]


def stay(a):
    return pltpu.with_memory_space_constraint(a, pltpu.HBM)


def near_by(a):
    return pltpu.with_memory_space_constraint(a, pltpu.VMEM)


def shards(
    residual, toa_error, basis_rows, efac_table, equad_table, pulsar, backend, counts, owner_slot
):
    far, near = lax.axis_size(FAR), lax.axis_size(NEAR)
    tiles, cols, rows = basis_rows.shape
    own = jnp.transpose(basis_rows, (1, 0, 2))
    other = lax.ppermute(own, "rep", SWAP)
    message = far + far * WIDE
    line = lambda a: a.reshape(1, -1)
    ints = [line(a) for a in (pulsar, backend, counts, owner_slot)]
    left, acc = pl.pallas_call(
        functools.partial(own_kernel, near, far),
        out_shape=(
            jax.ShapeDtypeStruct((tiles, 2 * SECOND, rows), BF16),
            jax.ShapeDtypeStruct((near * message, LANES), F32),
        ),
        in_specs=[HBM] * 9,
        out_specs=tuple(vmem(2)),
        scratch_shapes=[pltpu.VMEM((1, tiles), jnp.int32)] * 4
        + [pltpu.VMEM((tiles, rows), F32)] * 2
        + [pltpu.VMEM(efac_table.shape[::-1], F32)] * 2
        + [
            pltpu.VMEM(own.shape, BF16),
            pltpu.SMEM((1, tiles), jnp.int32),
            pltpu.VMEM((tiles, rows), F32),
            pltpu.VMEM((tiles, rows), BF16),
            pltpu.SemaphoreType.DMA((9,)),
            pltpu.SemaphoreType.DMA((tiles // GROUP,)),
        ],
        compiler_params=pltpu.CompilerParams(vmem_limit_bytes=32 << 20),
        cost_estimate=pl.CostEstimate(flops=2 * 10**9, transcendentals=0, bytes_accessed=10**7),
        name="own",
    )(*map(stay, (*ints, residual, toa_error, efac_table.T, equad_table.T, own)))
    sent, _ = pl.pallas_call(
        functools.partial(cross_kernel, near, far),
        out_shape=(
            pltpu.VMEM((near, message, LANES), BF16),
            pltpu.VMEM((near * message, LANES), F32),
        ),
        in_specs=[SMEM] + vmem(3),
        out_specs=tuple(vmem(2)),
        input_output_aliases={2: 1},
        compiler_params=pltpu.CompilerParams(vmem_limit_bytes=32 << 20),
        name="cross",
    )(ints[0], left, acc, other)
    got = lax.all_to_all(sent, NEAR, 0, 0, tiled=True)
    sent = pl.pallas_call(
        functools.partial(near_kernel, far),
        out_shape=pltpu.VMEM((far, WHITE + SECOND, LANES), BF16),
        in_specs=vmem(1),
        out_specs=vmem(1)[0],
        scratch_shapes=[pltpu.VMEM((far * WIDE + 8, LANES), F32)],
        name="near_sum",
    )(near_by(got))
    got = lax.all_to_all(sent, FAR, 0, 0, tiled=True)
    mine = pl.pallas_call(
        far_kernel,
        out_shape=pltpu.VMEM((SECOND + tiles, LANES), F32),
        in_specs=vmem(1),
        out_specs=vmem(1)[0],
        name="far_sum",
    )(near_by(got))
    theirs = lax.ppermute(mine, "rep", SWAP)
    gram, projection, whitened = pl.pallas_call(
        join_kernel,
        out_shape=(
            jax.ShapeDtypeStruct((cols, 1, 2 * cols), F32),
            jax.ShapeDtypeStruct((1, cols), F32),
            jax.ShapeDtypeStruct((tiles, rows), F32),
        ),
        in_specs=vmem(2),
        out_specs=tuple(vmem(3)),
        name="join",
    )(near_by(mine), near_by(theirs))
    return jnp.transpose(gram, (1, 2, 0)), projection, whitened


def solution(mesh):
    split = Mesh(
        mesh.devices.reshape(8, 4, 4, mesh.shape["rep"]), ("toa_0", "toa_1", "toa_2", "rep")
    )
    placed = (
        P(TOA, None),
        P(TOA, None),
        P(TOA, "rep", None),
        P(),
        P(),
        P(TOA),
        P(TOA),
        P(TOA),
        P(TOA),
    )
    return jax.shard_map(
        shards,
        mesh=split,
        in_specs=placed,
        out_specs=(P(TOA, None, "rep"), P(TOA, "rep"), P(TOA, None)),
        check_vma=False,
    )
```

```python
import functools

import jax
import jax.numpy as jnp
from jax import lax
from jax.experimental import pallas as pl
from jax.experimental.pallas import tpu as pltpu
from jax.sharding import Mesh
from jax.sharding import PartitionSpec as P

TOA = ("toa_0", "toa_1", "toa_2")
FAR, NEAR = "toa_0", ("toa_1", "toa_2")
BF16, F32 = jnp.bfloat16, jnp.float32
LANES = 128
GROUP = 16

PART = 25
WIDE = PART + 1
SECOND = 32
OWN = 2 * PART
OWN2 = OWN + SECOND
USED = OWN2 + WIDE
PIECE = 18
PLACE = 126
LAST_PLACE = 124
WHITE = 16


def dot(a, b, dims=((1,), (0,)), **kw):
    return lax.dot_general(a, b, (dims, ((), ())), preferred_element_type=F32, **kw)


def iota(shape, dim):
    return lax.broadcasted_iota(jnp.int32, shape, dim)


def as_column(row, lanes):
    square = jnp.broadcast_to(row, (LANES, row.shape[1])).T
    return jnp.concatenate([square] * (lanes // LANES), axis=1)


def base_row(p, near, message, head):
    return (p % near) * message + head + (p // near) * WIDE


def split(value):
    lane = iota(value.shape, 1)
    rest = value - value.astype(BF16).astype(F32)
    first = pltpu.roll(rest, LANES - OWN - 1, 1)
    second = pltpu.roll(rest, LANES - (OWN2 + 1 - PART), 1)
    return jnp.where(lane < PART, first, jnp.where(lane < OWN, second, value))


def joined(value):
    lane = iota(value.shape, 1)
    first = pltpu.roll(value, OWN + 1, 1)
    second = pltpu.roll(value, OWN2 + 1 - PART, 1)
    return value + jnp.where(lane < OWN2, first, second)


def message_rows(far):
    rows = far + (far - 1) * WIDE
    return rows + -rows % 8


def own_kernel(
    near, far, pulsar_in, backend_in, counts_in, slot_in, residual_in, error_in, efac_in, equad_in,
    own_in, left_out, acc,
    pulsar, backend, counts, slot, residual, error, efac_t, equad_t, own, pulsar_sm,
    weight_vm, wres_vm, sems, own_sems,
):
    cols, tiles, rows = own.shape
    block = far + far * WIDE
    pulsars, backends = efac_t.shape[1], efac_t.shape[0]
    pairs = (
        (pulsar_in, pulsar), (backend_in, backend), (counts_in, counts), (slot_in, slot),
        (residual_in, residual), (error_in, error), (efac_in, efac_t), (equad_in, equad_t),
        (pulsar_in, pulsar_sm),
    )
    copies = [pltpu.make_async_copy(a, b, sems.at[i]) for i, (a, b) in enumerate(pairs)]

    def own_copy(g):
        here = pl.ds(pl.multiple_of(g * GROUP, GROUP), GROUP)
        return pltpu.make_async_copy(own_in.at[:, here, :], own.at[:, here, :], own_sems.at[g])

    for copy in copies:
        copy.start()
    for g in range(tiles // GROUP):
        own_copy(g).start()
    acc[...] = jnp.zeros_like(acc)
    for copy in copies:
        copy.wait()

    of_pulsar = (iota((pulsars, tiles), 0) == pulsar[...]).astype(F32)
    of_backend = (iota((backends, tiles), 0) == backend[...]).astype(F32)
    high = dict(precision=lax.Precision.HIGHEST)
    factor = jnp.sum(dot(efac_t[...], of_pulsar, **high) * of_backend, axis=0, keepdims=True)
    floor = jnp.sum(dot(equad_t[...], of_pulsar, **high) * of_backend, axis=0, keepdims=True)
    factor2 = as_column(factor * factor, rows)
    floor2 = as_column(floor * floor, rows)
    count = as_column(counts[...].astype(F32), rows)
    valid = iota((tiles, rows), 1).astype(F32) < count
    weight = jnp.where(valid, 1.0 / (factor2 * error[...] ** 2 + floor2), 0.0)
    weight_vm[...] = weight
    wres_vm[...] = (weight * residual[...]).astype(BF16)
    white = jnp.sqrt(weight) * residual[...]
    white = jnp.where(lax.axis_index("rep") == 0, white[:, :LANES], white[:, LANES:])

    me = lax.axis_index("toa_1") * lax.axis_size("toa_2") + lax.axis_index("toa_2")
    dest = slot[...] // tiles
    place = (slot[...] % tiles).astype(F32)
    order = (dest % near) * far + dest // near
    moved = (iota((tiles, tiles), 0) == order).astype(BF16)
    white_to = dot(moved, white.astype(BF16))
    place_to = dot(moved, as_column(place, LANES).astype(BF16))
    place_to = jnp.where(iota(place_to.shape, 1) == PLACE, place_to, 0.0)
    for n in range(near):
        at = n * block
        acc[at : at + far, :] = white_to[n * far : (n + 1) * far, :]
        acc[pl.ds(at + far + me, far, stride=WIDE), :] = place_to[n * far : (n + 1) * far, :]

    lefts = 2 * SECOND
    lane, row = iota((SECOND, lefts), 1), iota((SECOND, lefts), 0)
    lower = (row > 0) & (lane < row) & (lane < PART)
    projected = (row == 0) & (((lane > 0) & (lane < WIDE)) | (lane > SECOND))
    kept = ((row > 0) & (lane != SECOND)) | projected
    is_wres = iota((GROUP, rows), 0) == 0

    def turn(g, carry):
        t0 = pl.multiple_of(g * GROUP, GROUP)
        here = pl.ds(t0, GROUP)
        own_copy(g).wait()
        none = lambda n: jnp.zeros((n, GROUP, rows), BF16)
        slabs = [
            none(1),
            own[:PART, here, :],
            none(SECOND - WIDE),
            wres_vm[here, :].reshape(1, GROUP, rows),
            own[PART:, here, :],
            none(SECOND - WIDE),
        ]
        turned = pltpu.einshape("ktr->tkr", jnp.concatenate(slabs, axis=0))
        group_weight = weight_vm[here, :]
        for u in range(GROUP):
            right = turned[u]
            left = (right.astype(F32) * group_weight[u : u + 1, :]).astype(BF16)
            middle = slice(SECOND, SECOND + GROUP)
            middle = jnp.where(is_wres, right[middle], left[middle])
            left = jnp.concatenate([left[:SECOND], middle, left[SECOND + GROUP :]], axis=0)
            left_out[t0 + u] = left
            out = dot(left, right, ((1,), (1,)))
            low, high = out[:SECOND], out[SECOND:]
            moved = jnp.concatenate([high[:, SECOND + 1 :], high[:, : SECOND + 1]], axis=1)
            value = jnp.where(lower, moved, jnp.where(projected, high, low))
            value = jnp.where(kept, value, 0.0)
            base = base_row(pulsar_sm[0, t0 + u], near, block, far)
            acc[pl.ds(base, WIDE), OWN:USED] += value[:WIDE, : USED - OWN]
        return carry

    lax.fori_loop(0, tiles // GROUP, turn, 0)
    for n in range(near):
        here = pl.ds(n * block + far, far, stride=WIDE)
        acc[here, :] = split(acc[here, :])


def cross_kernel(near, far, pulsar_sm, left, acc_in, other, out, acc):
    cols, tiles, rows = other.shape
    block = far + far * WIDE
    message = out.shape[1]
    core = lax.axis_index("rep")
    lane, row = iota((SECOND, cols), 1), iota((SECOND, cols), 0)
    second = (lane >= PART) & (row > 0)

    def turn(g, carry):
        t0 = pl.multiple_of(g * GROUP, GROUP)
        here = pl.ds(t0, GROUP)
        slabs = [other[pl.ds(PART * core, PART), here, :], other[pl.ds(PART - PART * core, PART), here, :]]
        turned = pltpu.einshape("ktr->tkr", jnp.concatenate(slabs, axis=0))
        for u in range(GROUP):
            product = dot(left[t0 + u], turned[u], ((1,), (1,)))
            value = jnp.where(second, product[SECOND:], product[:SECOND])
            base = base_row(pulsar_sm[0, t0 + u], near, block, far)
            acc[pl.ds(base, WIDE), :cols] += value[:WIDE]
        return carry

    lax.fori_loop(0, tiles // GROUP, turn, 0)

    lane = iota((WIDE, LANES), 1)

    def pack(n, carry):
        at = pl.multiple_of(n * block, 8)
        last = acc[pl.ds(at + far + (far - 1) * WIDE, WIDE), :]
        for i in range(far - 1):
            here = pl.ds(at + far + i * WIDE, WIDE)
            if i < USED // PIECE:
                moved = pltpu.roll(last, USED - i * PIECE, 1)
                acc[here, USED : USED + PIECE] = moved[:, USED : USED + PIECE]
            else:
                moved = pltpu.roll(last, LANES - (PLACE - LAST_PLACE), 1)
                acc[here, LAST_PLACE : LAST_PLACE + 1] = moved[:, LAST_PLACE : LAST_PLACE + 1]
        out[n] = acc[pl.ds(at, message), :].astype(BF16)
        return carry

    lax.fori_loop(0, near, pack, 0, unroll=4)


def near_kernel(far, got, out, total):
    near = got.shape[0]
    part = got[:, :far, :].astype(F32)
    out[:, :near, :] = jnp.swapaxes(part, 0, 1).astype(BF16)
    summed = got[0, far:, :].astype(F32)
    for n in range(1, near):
        summed = summed + got[n, far:, :].astype(F32)
    total[: summed.shape[0], :] = summed
    total[summed.shape[0] :, :] = jnp.zeros((total.shape[0] - summed.shape[0], LANES), F32)
    lane, row = iota((SECOND, LANES), 1), iota((SECOND, LANES), 0)
    last = jnp.zeros((SECOND, LANES), F32)
    for f in range(far):
        if f < far - 1:
            block = total[f * WIDE : f * WIDE + SECOND, :]
            if f < USED // PIECE:
                moved = pltpu.roll(block, LANES - (USED - f * PIECE), 1)
                last = jnp.where((lane >= f * PIECE) & (lane < (f + 1) * PIECE), moved, last)
            else:
                last = jnp.where(lane == PLACE, pltpu.roll(block, PLACE - LAST_PLACE, 1), last)
        else:
            block = last
        whole = split(joined(block))
        whole = jnp.where(lane == PLACE, block, whole)
        out[f, WHITE:, :] = jnp.where(row == 0, whole, block).astype(BF16)


def far_kernel(got, out):
    far, near = got.shape[0], WHITE
    tiles = far * near
    total = got[0, WHITE:, :].astype(F32)
    for f in range(1, far):
        total = total + got[f, WHITE:, :].astype(F32)
    out[:SECOND, :] = total
    lane = iota((near, LANES), 1)
    puts = []
    for f in range(far):
        value = got[f, WHITE : WHITE + near, :].astype(F32)
        place = jnp.sum(jnp.where(lane == PLACE, value, 0.0), axis=1, keepdims=True)
        puts.append((lane.astype(F32) == place).astype(F32))
    put = jnp.concatenate(puts, axis=0).astype(BF16)
    out[SECOND:, :] = dot(put, got[:, :near, :].reshape(tiles, LANES), ((0,), (0,)))


def join_kernel(mine_in, theirs_in, gram, proj, white, mine_t, theirs_t):
    lane, row = iota((SECOND, LANES), 1), iota((SECOND, LANES), 0)
    mine = mine_in[1 : SECOND + 1, :]

    def square(a):
        return jnp.concatenate([a, jnp.zeros((LANES - SECOND, LANES), F32)], axis=0).T

    mine_t[...] = square(mine)
    theirs_t[...] = square(theirs_in[1 : SECOND + 1, :])
    low = pltpu.roll(mine, LANES - OWN - 1, 1)
    first = jnp.where(lane >= row, low, mine_t[OWN + 1 : OWN + SECOND + 1, :])
    high = pltpu.roll(mine, LANES - OWN, 1)
    second = jnp.where(lane <= row, high, mine_t[OWN : OWN + SECOND, :])
    turned = mine_t[OWN2 + 1 : OWN2 + SECOND + 1, :]
    theirs_0 = theirs_t[:SECOND, :]
    theirs_1 = theirs_t[PART : PART + SECOND, :]

    def laid(pieces):
        value = jnp.zeros((SECOND, LANES), F32)
        for source, start, to in pieces:
            moved = pltpu.roll(source, (to - start) % LANES, 1) if to != start else source
            value = jnp.where((lane >= to) & (lane < to + PART), moved, value)
        return value

    def write(own, low, high):
        top = [(first, 0, own), (mine, OWN2 + 1, own + PART)]
        under = [(turned, 0, own), (second, 0, own + PART)]
        if own == 0:
            top += [(mine, 0, low), (theirs_1, 0, high)]
            under += [(theirs_0, 0, low), (mine, PART, high)]
        else:
            top += [(theirs_0, 0, low), (mine, 0, high)]
            under += [(mine, PART, low), (theirs_1, 0, high)]
        gram[:PART, 0, :] = laid(top)[:PART, : 4 * PART]
        gram[PART:, 0, :] = laid(under)[:PART, : 4 * PART]
        halves = (mine_in, theirs_in) if own == 0 else (theirs_in, mine_in)
        for i, half in enumerate(halves):
            white[:, i * LANES : (i + 1) * LANES] = half[SECOND:, :]

    core = lax.axis_index("rep")

    @pl.when(core == 0)
    def _():
        write(0, 2 * PART, 3 * PART)

    @pl.when(core == 1)
    def _():
        write(2 * PART, 0, PART)

    sums = joined(mine_in[:SECOND, :])
    proj[...] = laid([(sums, OWN + 1, 0), (sums, OWN2 + 1, PART)])[:1, : 2 * PART]


def vmem(n):
    return [pl.BlockSpec(memory_space=pltpu.VMEM)] * n


SMEM = pl.BlockSpec(memory_space=pltpu.SMEM)
HBM = pl.BlockSpec(memory_space=pltpu.HBM)
SWAP = [(0, 1), (1, 0)]


def stay(a):
    return pltpu.with_memory_space_constraint(a, pltpu.HBM)


def near_by(a):
    return pltpu.with_memory_space_constraint(a, pltpu.VMEM)


def shards(
    residual, toa_error, basis_rows, efac_table, equad_table, pulsar, backend, counts, owner_slot
):
    far, near = lax.axis_size(FAR), lax.axis_size(NEAR)
    tiles, cols, rows = basis_rows.shape
    own = jnp.transpose(basis_rows, (1, 0, 2))
    other = lax.ppermute(own, "rep", SWAP)
    block = far + far * WIDE
    message = message_rows(far)
    line = lambda a: a.reshape(1, -1)
    ints = [line(a) for a in (pulsar, backend, counts, owner_slot)]
    left, acc = pl.pallas_call(
        functools.partial(own_kernel, near, far),
        out_shape=(
            jax.ShapeDtypeStruct((tiles, 2 * SECOND, rows), BF16),
            jax.ShapeDtypeStruct((near * block, LANES), F32),
        ),
        in_specs=[HBM] * 9,
        out_specs=tuple(vmem(2)),
        scratch_shapes=[pltpu.VMEM((1, tiles), jnp.int32)] * 4
        + [pltpu.VMEM((tiles, rows), F32)] * 2
        + [pltpu.VMEM(efac_table.shape[::-1], F32)] * 2
        + [
            pltpu.VMEM(own.shape, BF16),
            pltpu.SMEM((1, tiles), jnp.int32),
            pltpu.VMEM((tiles, rows), F32),
            pltpu.VMEM((tiles, rows), BF16),
            pltpu.SemaphoreType.DMA((9,)),
            pltpu.SemaphoreType.DMA((tiles // GROUP,)),
        ],
        compiler_params=pltpu.CompilerParams(vmem_limit_bytes=32 << 20),
        cost_estimate=pl.CostEstimate(flops=2 * 10**9, transcendentals=0, bytes_accessed=10**7),
        name="own",
    )(*map(stay, (*ints, residual, toa_error, efac_table.T, equad_table.T, own)))
    sent, _ = pl.pallas_call(
        functools.partial(cross_kernel, near, far),
        out_shape=(
            pltpu.VMEM((near, message, LANES), BF16),
            pltpu.VMEM((near * block, LANES), F32),
        ),
        in_specs=[SMEM] + vmem(3),
        out_specs=tuple(vmem(2)),
        input_output_aliases={2: 1},
        compiler_params=pltpu.CompilerParams(vmem_limit_bytes=32 << 20),
        name="cross",
    )(ints[0], left, acc, other)
    got = lax.all_to_all(sent, NEAR, 0, 0, tiled=True)
    sent = pl.pallas_call(
        functools.partial(near_kernel, far),
        out_shape=pltpu.VMEM((far, WHITE + SECOND, LANES), BF16),
        in_specs=vmem(1),
        out_specs=vmem(1)[0],
        scratch_shapes=[pltpu.VMEM((message, LANES), F32)],
        name="near_sum",
    )(near_by(got))
    got = lax.all_to_all(sent, FAR, 0, 0, tiled=True)
    mine = pl.pallas_call(
        far_kernel,
        out_shape=pltpu.VMEM((SECOND + tiles, LANES), F32),
        in_specs=vmem(1),
        out_specs=vmem(1)[0],
        name="far_sum",
    )(near_by(got))
    theirs = lax.ppermute(mine, "rep", SWAP)
    gram, projection, whitened = pl.pallas_call(
        join_kernel,
        out_shape=(
            jax.ShapeDtypeStruct((cols, 1, 2 * cols), F32),
            jax.ShapeDtypeStruct((1, cols), F32),
            jax.ShapeDtypeStruct((tiles, rows), F32),
        ),
        in_specs=vmem(2),
        out_specs=tuple(vmem(3)),
        scratch_shapes=[pltpu.VMEM((LANES, LANES), F32)] * 2,
        name="join",
    )(near_by(mine), near_by(theirs))
    return jnp.transpose(gram, (1, 2, 0)), projection, whitened


def solution(mesh):
    split = Mesh(
        mesh.devices.reshape(8, 4, 4, mesh.shape["rep"]), ("toa_0", "toa_1", "toa_2", "rep")
    )
    placed = (
        P(TOA, None),
        P(TOA, None),
        P(TOA, "rep", None),
        P(),
        P(),
        P(TOA),
        P(TOA),
        P(TOA),
        P(TOA),
    )
    return jax.shard_map(
        shards,
        mesh=split,
        in_specs=placed,
        out_specs=(P(TOA, None, "rep"), P(TOA, "rep"), P(TOA, None)),
        check_vma=False,
    )
```

```python
import functools

import jax
import jax.numpy as jnp
from jax import lax
from jax.experimental import pallas as pl
from jax.experimental.pallas import tpu as pltpu
from jax.sharding import Mesh
from jax.sharding import PartitionSpec as P

TOA = ("toa_0", "toa_1", "toa_2")
FAR, NEAR = "toa_0", ("toa_1", "toa_2")
BF16, F32 = jnp.bfloat16, jnp.float32
LANES = 128
GROUP = 16

PART = 25
WIDE = PART + 1
SECOND = 32
OWN = 2 * PART
OWN2 = OWN + SECOND
USED = OWN2 + WIDE
PIECE = 18
PLACE = 126
LAST_PLACE = 124
WHITE = 16


def dot(a, b, dims=((1,), (0,)), **kw):
    return lax.dot_general(a, b, (dims, ((), ())), preferred_element_type=F32, **kw)


def iota(shape, dim):
    return lax.broadcasted_iota(jnp.int32, shape, dim)


def as_column(row, lanes):
    square = jnp.broadcast_to(row, (LANES, row.shape[1])).T
    return jnp.concatenate([square] * (lanes // LANES), axis=1)


def base_row(p, near, message, head):
    return (p & (near - 1)) * message + head + (p >> (near.bit_length() - 1)) * WIDE


def split(value):
    lane = iota(value.shape, 1)
    rest = value - value.astype(BF16).astype(F32)
    first = pltpu.roll(rest, LANES - OWN - 1, 1)
    second = pltpu.roll(rest, LANES - (OWN2 + 1 - PART), 1)
    return jnp.where(lane < PART, first, jnp.where(lane < OWN, second, value))


def joined(value):
    lane = iota(value.shape, 1)
    first = pltpu.roll(value, OWN + 1, 1)
    second = pltpu.roll(value, OWN2 + 1 - PART, 1)
    return value + jnp.where(lane < OWN2, first, second)


def message_rows(far):
    rows = far + (far - 1) * WIDE
    return rows + -rows % 8


def own_kernel(
    near, far, pulsar_in, backend_in, counts_in, slot_in, residual_in, error_in, efac_in, equad_in,
    own_in, left_out, acc,
    pulsar, backend, counts, slot, residual, error, efac_t, equad_t, own, pulsar_sm,
    weight_vm, wres_vm, sems, own_sems,
):
    cols, tiles, rows = own.shape
    block = far + far * WIDE
    pulsars, backends = efac_t.shape[1], efac_t.shape[0]
    pairs = (
        (pulsar_in, pulsar), (backend_in, backend), (efac_in, efac_t), (equad_in, equad_t),
        (counts_in, counts), (error_in, error), (residual_in, residual), (slot_in, slot),
        (pulsar_in, pulsar_sm),
    )
    copies = [pltpu.make_async_copy(a, b, sems.at[i]) for i, (a, b) in enumerate(pairs)]

    def own_copy(g):
        here = pl.ds(pl.multiple_of(g * GROUP, GROUP), GROUP)
        return pltpu.make_async_copy(own_in.at[:, here, :], own.at[:, here, :], own_sems.at[g])

    for copy in copies:
        copy.start()
    for g in range(tiles // GROUP):
        own_copy(g).start()
    acc[...] = jnp.zeros_like(acc)
    for copy in copies[:4]:
        copy.wait()

    of_pulsar = (iota((pulsars, tiles), 0) == pulsar[...]).astype(F32)
    of_backend = (iota((backends, tiles), 0) == backend[...]).astype(F32)
    high = dict(precision=lax.Precision.HIGHEST)
    factor = jnp.sum(dot(efac_t[...], of_pulsar, **high) * of_backend, axis=0, keepdims=True)
    floor = jnp.sum(dot(equad_t[...], of_pulsar, **high) * of_backend, axis=0, keepdims=True)
    factor2 = as_column(factor * factor, rows)
    floor2 = as_column(floor * floor, rows)
    for copy in copies[4:7]:
        copy.wait()
    count = as_column(counts[...].astype(F32), rows)
    valid = iota((tiles, rows), 1).astype(F32) < count
    weight = jnp.where(valid, 1.0 / (factor2 * error[...] ** 2 + floor2), 0.0)
    weight_vm[...] = weight
    wres_vm[...] = (weight * residual[...]).astype(BF16)
    white = jnp.sqrt(weight) * residual[...]
    white = jnp.where(lax.axis_index("rep") == 0, white[:, :LANES], white[:, LANES:])

    me = lax.axis_index("toa_1") * lax.axis_size("toa_2") + lax.axis_index("toa_2")
    copies[7].wait()
    dest = slot[...] // tiles
    place = (slot[...] % tiles).astype(F32)
    order = (dest % near) * far + dest // near
    moved = (iota((tiles, tiles), 0) == order).astype(BF16)
    white_to = dot(moved, white.astype(BF16))
    place_to = dot(moved, as_column(place, LANES).astype(BF16))
    place_to = jnp.where(iota(place_to.shape, 1) == PLACE, place_to, 0.0)
    for n in range(near):
        at = n * block
        acc[at : at + far, :] = white_to[n * far : (n + 1) * far, :]
        acc[pl.ds(at + far + me, far, stride=WIDE), :] = place_to[n * far : (n + 1) * far, :]

    copies[8].wait()

    lefts = 2 * SECOND
    lane, row = iota((SECOND, lefts), 1), iota((SECOND, lefts), 0)
    lower = (row > 0) & (lane < row) & (lane < PART)
    projected = row == 0
    is_wres = iota((GROUP, rows), 0) == 0
    beyond = jnp.zeros((SECOND, SECOND + 1), F32)

    def turn(g, carry):
        t0 = pl.multiple_of(g * GROUP, GROUP)
        here = pl.ds(t0, GROUP)
        own_copy(g).wait()
        none = lambda n: jnp.zeros((n, GROUP, rows), BF16)
        slabs = [
            none(1),
            own[:PART, here, :],
            none(SECOND - WIDE),
            wres_vm[here, :].reshape(1, GROUP, rows),
            own[PART:, here, :],
            none(SECOND - WIDE),
        ]
        turned = pltpu.einshape("ktr->tkr", jnp.concatenate(slabs, axis=0))
        group_weight = weight_vm[here, :]
        for u in range(GROUP):
            right = turned[u]
            left = (right.astype(F32) * group_weight[u : u + 1, :]).astype(BF16)
            middle = slice(SECOND, SECOND + GROUP)
            middle = jnp.where(is_wres, right[middle], left[middle])
            left = jnp.concatenate([left[:SECOND], middle, left[SECOND + GROUP :]], axis=0)
            left_out[t0 + u] = left
            out = dot(left, right, ((1,), (1,)))
            low, high = out[:SECOND], out[SECOND:]
            moved = jnp.concatenate([high[:, SECOND + 1 :], beyond], axis=1)
            value = jnp.where(lower, moved, jnp.where(projected, high, low))
            base = base_row(pulsar_sm[0, t0 + u], near, block, far)
            acc[pl.ds(base, WIDE), OWN:USED] += value[:WIDE, : USED - OWN]
        return carry

    lax.fori_loop(0, tiles // GROUP, turn, 0)
    for n in range(near):
        here = pl.ds(n * block + far, far, stride=WIDE)
        acc[here, :] = split(acc[here, :])


def cross_kernel(near, far, pulsar, left, acc_in, other, out, acc):
    cols, tiles, rows = other.shape
    block = far + far * WIDE
    message = out.shape[1]
    core = lax.axis_index("rep")
    lane, row = iota((SECOND, cols), 1), iota((SECOND, cols), 0)
    second = (lane >= PART) & (row > 0)
    bases = base_row(pulsar[...], near, block, far).astype(F32)
    tile = iota(bases.shape, 1)

    def turn(g, carry):
        t0 = pl.multiple_of(g * GROUP, GROUP)
        here = pl.ds(t0, GROUP)
        slabs = [other[pl.ds(PART * core, PART), here, :], other[pl.ds(PART - PART * core, PART), here, :]]
        turned = pltpu.einshape("ktr->tkr", jnp.concatenate(slabs, axis=0))
        for u in range(GROUP):
            product = dot(left[t0 + u], turned[u], ((1,), (1,)))
            value = jnp.where(second, product[SECOND:], product[:SECOND])
            base = jnp.sum(jnp.where(tile == t0 + u, bases, 0.0)).astype(jnp.int32)
            acc[pl.ds(base, WIDE), :cols] += value[:WIDE]
        return carry

    lax.fori_loop(0, tiles // GROUP, turn, 0)

    lane = iota((WIDE, LANES), 1)
    spare = (lane >= USED) & (lane < USED + PIECE)

    def fold(n, carry):
        at = n * block + far
        last = acc[pl.ds(at + (far - 1) * WIDE, SECOND), :].astype(BF16)
        for i in range(far - 1):
            here = acc.at[pl.ds(at + i * WIDE, WIDE), :]
            if i < USED // PIECE:
                pltpu.store(here, pltpu.roll(last, USED - i * PIECE, 1).astype(F32)[:WIDE], mask=spare)
            else:
                place = pltpu.roll(last, LANES - (PLACE - LAST_PLACE), 1).astype(F32)[:WIDE]
                pltpu.store(here, place, mask=lane == LAST_PLACE)
        return carry

    def convert(n, carry):
        out[n] = acc[pl.ds(pl.multiple_of(n * block, 8), message), :].astype(BF16)
        return carry

    lax.fori_loop(0, near, fold, 0, unroll=4)
    lax.fori_loop(0, near, convert, 0, unroll=2)


def near_kernel(far, got, out, total):
    near = got.shape[0]
    part = got[:, :far, :].astype(F32)
    out[:, :near, :] = jnp.swapaxes(part, 0, 1).astype(BF16)
    summed = got[0, far:, :].astype(F32)
    for n in range(1, near):
        summed = summed + got[n, far:, :].astype(F32)
    total[: summed.shape[0], :] = summed
    total[summed.shape[0] :, :] = jnp.zeros((total.shape[0] - summed.shape[0], LANES), F32)
    lane, row = iota((SECOND, LANES), 1), iota((SECOND, LANES), 0)
    last = jnp.zeros((SECOND, LANES), F32)
    for f in range(far):
        if f < far - 1:
            block = total[f * WIDE : f * WIDE + SECOND, :]
            if f < USED // PIECE:
                moved = pltpu.roll(block, LANES - (USED - f * PIECE), 1)
                last = jnp.where((lane >= f * PIECE) & (lane < (f + 1) * PIECE), moved, last)
            else:
                last = jnp.where(lane == PLACE, pltpu.roll(block, PLACE - LAST_PLACE, 1), last)
        else:
            block = last
        whole = split(joined(block))
        whole = jnp.where(lane == PLACE, block, whole)
        out[f, WHITE:, :] = jnp.where(row == 0, whole, block).astype(BF16)


def far_kernel(got, out):
    far, near = got.shape[0], WHITE
    tiles = far * near
    total = got[0, WHITE:, :].astype(F32)
    for f in range(1, far):
        total = total + got[f, WHITE:, :].astype(F32)
    out[:SECOND, :] = total
    lane = iota((near, LANES), 1)
    puts = []
    for f in range(far):
        value = got[f, WHITE : WHITE + near, :].astype(F32)
        place = jnp.sum(jnp.where(lane == PLACE, value, 0.0), axis=1, keepdims=True)
        puts.append((lane.astype(F32) == place).astype(F32))
    put = jnp.concatenate(puts, axis=0).astype(BF16)
    out[SECOND:, :] = dot(put, got[:, :near, :].reshape(tiles, LANES), ((0,), (0,)))


def join_kernel(mine_in, theirs_in, gram, proj, white, mine_t, theirs_t):
    lane, row = iota((SECOND, LANES), 1), iota((SECOND, LANES), 0)
    mine = mine_in[1 : SECOND + 1, :]

    def square(a):
        return jnp.concatenate([a, jnp.zeros((LANES - SECOND, LANES), F32)], axis=0).T

    mine_t[...] = square(mine)
    theirs_t[...] = square(theirs_in[1 : SECOND + 1, :])
    low = pltpu.roll(mine, LANES - OWN - 1, 1)
    first = jnp.where(lane >= row, low, mine_t[OWN + 1 : OWN + SECOND + 1, :])
    high = pltpu.roll(mine, LANES - OWN, 1)
    second = jnp.where(lane <= row, high, mine_t[OWN : OWN + SECOND, :])
    turned = mine_t[OWN2 + 1 : OWN2 + SECOND + 1, :]
    theirs_0 = theirs_t[:SECOND, :]
    theirs_1 = theirs_t[PART : PART + SECOND, :]

    def laid(pieces):
        value = jnp.zeros((SECOND, LANES), F32)
        for source, start, to in pieces:
            moved = pltpu.roll(source, (to - start) % LANES, 1) if to != start else source
            value = jnp.where((lane >= to) & (lane < to + PART), moved, value)
        return value

    def write(own, low, high):
        top = [(first, 0, own), (mine, OWN2 + 1, own + PART)]
        under = [(turned, 0, own), (second, 0, own + PART)]
        if own == 0:
            top += [(mine, 0, low), (theirs_1, 0, high)]
            under += [(theirs_0, 0, low), (mine, PART, high)]
        else:
            top += [(theirs_0, 0, low), (mine, 0, high)]
            under += [(mine, PART, low), (theirs_1, 0, high)]
        gram[:PART, 0, :] = laid(top)[:PART, : 4 * PART]
        gram[PART:, 0, :] = laid(under)[:PART, : 4 * PART]
        halves = (mine_in, theirs_in) if own == 0 else (theirs_in, mine_in)
        for i, half in enumerate(halves):
            white[:, i * LANES : (i + 1) * LANES] = half[SECOND:, :]

    core = lax.axis_index("rep")

    @pl.when(core == 0)
    def _():
        write(0, 2 * PART, 3 * PART)

    @pl.when(core == 1)
    def _():
        write(2 * PART, 0, PART)

    sums = joined(mine_in[:SECOND, :])
    proj[...] = laid([(sums, OWN + 1, 0), (sums, OWN2 + 1, PART)])[:1, : 2 * PART]


def vmem(n):
    return [pl.BlockSpec(memory_space=pltpu.VMEM)] * n


HBM = pl.BlockSpec(memory_space=pltpu.HBM)
SWAP = [(0, 1), (1, 0)]


def stay(a):
    return pltpu.with_memory_space_constraint(a, pltpu.HBM)


def near_by(a):
    return pltpu.with_memory_space_constraint(a, pltpu.VMEM)


def shards(
    residual, toa_error, basis_rows, efac_table, equad_table, pulsar, backend, counts, owner_slot
):
    far, near = lax.axis_size(FAR), lax.axis_size(NEAR)
    tiles, cols, rows = basis_rows.shape
    own = jnp.transpose(basis_rows, (1, 0, 2))
    other = lax.ppermute(own, "rep", SWAP)
    block = far + far * WIDE
    message = message_rows(far)
    line = lambda a: a.reshape(1, -1)
    ints = [line(a) for a in (pulsar, backend, counts, owner_slot)]
    left, acc = pl.pallas_call(
        functools.partial(own_kernel, near, far),
        out_shape=(
            jax.ShapeDtypeStruct((tiles, 2 * SECOND, rows), BF16),
            jax.ShapeDtypeStruct((near * block + 8, LANES), F32),
        ),
        in_specs=[HBM] * 9,
        out_specs=tuple(vmem(2)),
        scratch_shapes=[pltpu.VMEM((1, tiles), jnp.int32)] * 4
        + [pltpu.VMEM((tiles, rows), F32)] * 2
        + [pltpu.VMEM(efac_table.shape[::-1], F32)] * 2
        + [
            pltpu.VMEM(own.shape, BF16),
            pltpu.SMEM((1, tiles), jnp.int32),
            pltpu.VMEM((tiles, rows), F32),
            pltpu.VMEM((tiles, rows), BF16),
            pltpu.SemaphoreType.DMA((9,)),
            pltpu.SemaphoreType.DMA((tiles // GROUP,)),
        ],
        compiler_params=pltpu.CompilerParams(vmem_limit_bytes=32 << 20),
        cost_estimate=pl.CostEstimate(flops=2 * 10**9, transcendentals=0, bytes_accessed=10**7),
        name="own",
    )(*map(stay, (*ints, residual, toa_error, efac_table.T, equad_table.T, own)))
    sent, _ = pl.pallas_call(
        functools.partial(cross_kernel, near, far),
        out_shape=(
            pltpu.VMEM((near, message, LANES), BF16),
            pltpu.VMEM((near * block + 8, LANES), F32),
        ),
        in_specs=vmem(4),
        out_specs=tuple(vmem(2)),
        input_output_aliases={2: 1},
        compiler_params=pltpu.CompilerParams(vmem_limit_bytes=32 << 20),
        name="cross",
    )(ints[0], left, acc, other)
    got = lax.all_to_all(sent, NEAR, 0, 0, tiled=True)
    sent = pl.pallas_call(
        functools.partial(near_kernel, far),
        out_shape=pltpu.VMEM((far, WHITE + SECOND, LANES), BF16),
        in_specs=vmem(1),
        out_specs=vmem(1)[0],
        scratch_shapes=[pltpu.VMEM((message, LANES), F32)],
        name="near_sum",
    )(near_by(got))
    got = lax.all_to_all(sent, FAR, 0, 0, tiled=True)
    mine = pl.pallas_call(
        far_kernel,
        out_shape=pltpu.VMEM((SECOND + tiles, LANES), F32),
        in_specs=vmem(1),
        out_specs=vmem(1)[0],
        name="far_sum",
    )(near_by(got))
    theirs = lax.ppermute(mine, "rep", SWAP)
    gram, projection, whitened = pl.pallas_call(
        join_kernel,
        out_shape=(
            jax.ShapeDtypeStruct((cols, 1, 2 * cols), F32),
            jax.ShapeDtypeStruct((1, cols), F32),
            jax.ShapeDtypeStruct((tiles, rows), F32),
        ),
        in_specs=vmem(2),
        out_specs=tuple(vmem(3)),
        scratch_shapes=[pltpu.VMEM((LANES, LANES), F32)] * 2,
        name="join",
    )(near_by(mine), near_by(theirs))
    return jnp.transpose(gram, (1, 2, 0)), projection, whitened


def solution(mesh):
    split = Mesh(
        mesh.devices.reshape(8, 4, 4, mesh.shape["rep"]), ("toa_0", "toa_1", "toa_2", "rep")
    )
    placed = (
        P(TOA, None),
        P(TOA, None),
        P(TOA, "rep", None),
        P(),
        P(),
        P(TOA),
        P(TOA),
        P(TOA),
        P(TOA),
    )
    return jax.shard_map(
        shards,
        mesh=split,
        in_specs=placed,
        out_specs=(P(TOA, None, "rep"), P(TOA, "rep"), P(TOA, None)),
        check_vma=False,
    )
```

```python
import functools

import jax
import jax.numpy as jnp
from jax import lax
from jax.experimental import pallas as pl
from jax.experimental.pallas import tpu as pltpu
from jax.sharding import Mesh
from jax.sharding import PartitionSpec as P

TOA = ("toa_0", "toa_1", "toa_2")
FAR, NEAR = "toa_0", ("toa_1", "toa_2")
BF16, F32 = jnp.bfloat16, jnp.float32
LANES = 128
GROUP = 16

PART = 25
WIDE = PART + 1
SECOND = 32
OWN = 2 * PART
OWN2 = OWN + SECOND
USED = OWN2 + WIDE
PIECE = 18
PLACE = 126
LAST_PLACE = 124
WHITE = 16


def dot(a, b, dims=((1,), (0,)), **kw):
    return lax.dot_general(a, b, (dims, ((), ())), preferred_element_type=F32, **kw)


def iota(shape, dim):
    return lax.broadcasted_iota(jnp.int32, shape, dim)


def as_column(row, lanes):
    square = jnp.broadcast_to(row, (LANES, row.shape[1])).T
    return jnp.concatenate([square] * (lanes // LANES), axis=1)


def base_row(p, near, message, head):
    return (p & (near - 1)) * message + head + (p >> (near.bit_length() - 1)) * WIDE


def split(value):
    lane = iota(value.shape, 1)
    rest = value - value.astype(BF16).astype(F32)
    first = pltpu.roll(rest, LANES - OWN - 1, 1)
    second = pltpu.roll(rest, LANES - (OWN2 + 1 - PART), 1)
    return jnp.where(lane < PART, first, jnp.where(lane < OWN, second, value))


def joined(value):
    lane = iota(value.shape, 1)
    first = pltpu.roll(value, OWN + 1, 1)
    second = pltpu.roll(value, OWN2 + 1 - PART, 1)
    return value + jnp.where(lane < OWN2, first, second)


def message_rows(far):
    rows = far + (far - 1) * WIDE
    return rows + -rows % 8


def own_kernel(
    near, far, pulsar_in, backend_in, counts_in, slot_in, residual_in, error_in, efac_in, equad_in,
    own_in, left_out, acc,
    pulsar, backend, counts, slot, residual, error, efac_t, equad_t, own, pulsar_sm,
    weight_vm, wres_vm, sems, own_sems,
):
    cols, tiles, rows = own.shape
    block = far + far * WIDE
    pulsars, backends = efac_t.shape[1], efac_t.shape[0]
    pairs = (
        (pulsar_in, pulsar), (backend_in, backend), (efac_in, efac_t), (equad_in, equad_t),
        (counts_in, counts), (error_in, error), (residual_in, residual), (slot_in, slot),
        (pulsar_in, pulsar_sm),
    )
    copies = [pltpu.make_async_copy(a, b, sems.at[i]) for i, (a, b) in enumerate(pairs)]

    def own_copy(g):
        here = pl.ds(pl.multiple_of(g * GROUP, GROUP), GROUP)
        return pltpu.make_async_copy(own_in.at[:, here, :], own.at[:, here, :], own_sems.at[g])

    for copy in copies:
        copy.start()
    for g in range(tiles // GROUP):
        own_copy(g).start()
    acc[...] = jnp.zeros_like(acc)
    for copy in copies[:4]:
        copy.wait()

    of_pulsar = (iota((pulsars, tiles), 0) == pulsar[...]).astype(F32)
    of_backend = (iota((backends, tiles), 0) == backend[...]).astype(F32)
    high = dict(precision=lax.Precision.HIGHEST)
    factor = jnp.sum(dot(efac_t[...], of_pulsar, **high) * of_backend, axis=0, keepdims=True)
    floor = jnp.sum(dot(equad_t[...], of_pulsar, **high) * of_backend, axis=0, keepdims=True)
    factor2 = as_column(factor * factor, rows)
    floor2 = as_column(floor * floor, rows)
    for copy in copies[4:7]:
        copy.wait()
    count = as_column(counts[...].astype(F32), rows)
    valid = iota((tiles, rows), 1).astype(F32) < count
    weight = jnp.where(valid, 1.0 / (factor2 * error[...] ** 2 + floor2), 0.0)
    weight_vm[...] = weight
    wres_vm[...] = (weight * residual[...]).astype(BF16)
    white = jnp.sqrt(weight) * residual[...]
    white = jnp.where(lax.axis_index("rep") == 0, white[:, :LANES], white[:, LANES:])

    me = lax.axis_index("toa_1") * lax.axis_size("toa_2") + lax.axis_index("toa_2")
    copies[7].wait()
    dest = slot[...] // tiles
    place = (slot[...] % tiles).astype(F32)
    order = (dest % near) * far + dest // near
    moved = (iota((tiles, tiles), 0) == order).astype(BF16)
    white_to = dot(moved, white.astype(BF16))
    place_to = dot(moved, as_column(place, LANES).astype(BF16))
    place_to = jnp.where(iota(place_to.shape, 1) == PLACE, place_to, 0.0)
    for n in range(near):
        at = n * block
        acc[at : at + far, :] = white_to[n * far : (n + 1) * far, :]
        acc[pl.ds(at + far + me, far, stride=WIDE), :] = place_to[n * far : (n + 1) * far, :]

    copies[8].wait()

    lefts = 2 * SECOND
    lane, row = iota((SECOND, lefts), 1), iota((SECOND, lefts), 0)
    lower = (row > 0) & (lane < row) & (lane < PART)
    projected = row == 0
    is_wres = iota((GROUP, rows), 0) == 0
    beyond = jnp.zeros((SECOND, SECOND + 1), F32)

    def turn(g, carry):
        t0 = pl.multiple_of(g * GROUP, GROUP)
        here = pl.ds(t0, GROUP)
        own_copy(g).wait()
        none = lambda n: jnp.zeros((n, GROUP, rows), BF16)
        slabs = [
            none(1),
            own[:PART, here, :],
            none(SECOND - WIDE),
            wres_vm[here, :].reshape(1, GROUP, rows),
            own[PART:, here, :],
            none(SECOND - WIDE),
        ]
        turned = pltpu.einshape("ktr->tkr", jnp.concatenate(slabs, axis=0))
        group_weight = weight_vm[here, :]
        for u in range(GROUP):
            right = turned[u]
            left = (right.astype(F32) * group_weight[u : u + 1, :]).astype(BF16)
            middle = slice(SECOND, SECOND + GROUP)
            middle = jnp.where(is_wres, right[middle], left[middle])
            left = jnp.concatenate([left[:SECOND], middle, left[SECOND + GROUP :]], axis=0)
            left_out[t0 + u] = left
            out = dot(left, right, ((1,), (1,)))
            low, high = out[:SECOND], out[SECOND:]
            moved = jnp.concatenate([high[:, SECOND + 1 :], beyond], axis=1)
            value = jnp.where(lower, moved, jnp.where(projected, high, low))
            base = base_row(pulsar_sm[0, t0 + u], near, block, far)
            acc[pl.ds(base, WIDE), OWN:USED] += value[:WIDE, : USED - OWN]
        return carry

    lax.fori_loop(0, tiles // GROUP, turn, 0)
    for n in range(near):
        here = pl.ds(n * block + far, far, stride=WIDE)
        acc[here, :] = split(acc[here, :])


def cross_kernel(near, far, pulsar, left, acc_in, other, out, acc):
    cols, tiles, rows = other.shape
    block = far + far * WIDE
    message = out.shape[1]
    core = lax.axis_index("rep")
    lane, row = iota((SECOND, cols), 1), iota((SECOND, cols), 0)
    second = (lane >= PART) & (row > 0)
    bases = base_row(pulsar[...], near, block, far).astype(F32)
    tile = iota(bases.shape, 1)

    def turn(g, carry):
        t0 = pl.multiple_of(g * GROUP, GROUP)
        here = pl.ds(t0, GROUP)
        slabs = [other[pl.ds(PART * core, PART), here, :], other[pl.ds(PART - PART * core, PART), here, :]]
        turned = pltpu.einshape("ktr->tkr", jnp.concatenate(slabs, axis=0))
        for u in range(GROUP):
            product = dot(left[t0 + u], turned[u], ((1,), (1,)))
            value = jnp.where(second, product[SECOND:], product[:SECOND])
            base = jnp.sum(jnp.where(tile == t0 + u, bases, 0.0)).astype(jnp.int32)
            acc[pl.ds(base, WIDE), :cols] += value[:WIDE]
        return carry

    lax.fori_loop(0, tiles // GROUP, turn, 0, unroll=tiles // GROUP)

    lane = iota((WIDE, LANES), 1)
    spare = (lane >= USED) & (lane < USED + PIECE)

    def fold(n, carry):
        at = n * block + far
        last = acc[pl.ds(at + (far - 1) * WIDE, SECOND), :].astype(BF16)
        for i in range(far - 1):
            here = acc.at[pl.ds(at + i * WIDE, WIDE), :]
            if i < USED // PIECE:
                pltpu.store(here, pltpu.roll(last, USED - i * PIECE, 1).astype(F32)[:WIDE], mask=spare)
            else:
                place = pltpu.roll(last, LANES - (PLACE - LAST_PLACE), 1).astype(F32)[:WIDE]
                pltpu.store(here, place, mask=lane == LAST_PLACE)
        return carry

    def convert(n, carry):
        out[n] = acc[pl.ds(pl.multiple_of(n * block, 8), message), :].astype(BF16)
        return carry

    lax.fori_loop(0, near, fold, 0, unroll=8)
    lax.fori_loop(0, near, convert, 0, unroll=4)


def near_kernel(far, got, out, total):
    near = got.shape[0]
    part = got[:, :far, :].astype(F32)
    out[:, :near, :] = jnp.swapaxes(part, 0, 1).astype(BF16)
    summed = got[0, far:, :].astype(F32)
    for n in range(1, near):
        summed = summed + got[n, far:, :].astype(F32)
    total[: summed.shape[0], :] = summed
    total[summed.shape[0] :, :] = jnp.zeros((total.shape[0] - summed.shape[0], LANES), F32)
    lane, row = iota((SECOND, LANES), 1), iota((SECOND, LANES), 0)
    last = jnp.zeros((SECOND, LANES), F32)
    for f in range(far):
        if f < far - 1:
            block = total[f * WIDE : f * WIDE + SECOND, :]
            if f < USED // PIECE:
                moved = pltpu.roll(block, LANES - (USED - f * PIECE), 1)
                last = jnp.where((lane >= f * PIECE) & (lane < (f + 1) * PIECE), moved, last)
            else:
                last = jnp.where(lane == PLACE, pltpu.roll(block, PLACE - LAST_PLACE, 1), last)
        else:
            block = last
        whole = split(joined(block))
        whole = jnp.where(lane == PLACE, block, whole)
        out[f, WHITE:, :] = jnp.where(row == 0, whole, block).astype(BF16)


def far_kernel(got, out):
    far, near = got.shape[0], WHITE
    tiles = far * near
    total = got[0, WHITE:, :].astype(F32)
    for f in range(1, far):
        total = total + got[f, WHITE:, :].astype(F32)
    out[:SECOND, :] = total
    lane = iota((near, LANES), 1)
    puts = []
    for f in range(far):
        value = got[f, WHITE : WHITE + near, :].astype(F32)
        place = jnp.sum(jnp.where(lane == PLACE, value, 0.0), axis=1, keepdims=True)
        puts.append((lane.astype(F32) == place).astype(F32))
    put = jnp.concatenate(puts, axis=0).astype(BF16)
    out[SECOND:, :] = dot(put, got[:, :near, :].reshape(tiles, LANES), ((0,), (0,)))


def join_kernel(mine_in, theirs_in, gram, proj, white, mine_t, theirs_t):
    lane, row = iota((SECOND, LANES), 1), iota((SECOND, LANES), 0)
    mine = mine_in[1 : SECOND + 1, :]

    def square(a):
        return jnp.concatenate([a, jnp.zeros((LANES - SECOND, LANES), F32)], axis=0).T

    mine_t[...] = square(mine)
    theirs_t[...] = square(theirs_in[1 : SECOND + 1, :])
    low = pltpu.roll(mine, LANES - OWN - 1, 1)
    first = jnp.where(lane >= row, low, mine_t[OWN + 1 : OWN + SECOND + 1, :])
    high = pltpu.roll(mine, LANES - OWN, 1)
    second = jnp.where(lane <= row, high, mine_t[OWN : OWN + SECOND, :])
    turned = mine_t[OWN2 + 1 : OWN2 + SECOND + 1, :]
    theirs_0 = theirs_t[:SECOND, :]
    theirs_1 = theirs_t[PART : PART + SECOND, :]

    def laid(pieces):
        value = jnp.zeros((SECOND, LANES), F32)
        for source, start, to in pieces:
            moved = pltpu.roll(source, (to - start) % LANES, 1) if to != start else source
            value = jnp.where((lane >= to) & (lane < to + PART), moved, value)
        return value

    def write(own, low, high):
        top = [(first, 0, own), (mine, OWN2 + 1, own + PART)]
        under = [(turned, 0, own), (second, 0, own + PART)]
        if own == 0:
            top += [(mine, 0, low), (theirs_1, 0, high)]
            under += [(theirs_0, 0, low), (mine, PART, high)]
        else:
            top += [(theirs_0, 0, low), (mine, 0, high)]
            under += [(mine, PART, low), (theirs_1, 0, high)]
        gram[:PART, 0, :] = laid(top)[:PART, : 4 * PART]
        gram[PART:, 0, :] = laid(under)[:PART, : 4 * PART]
        halves = (mine_in, theirs_in) if own == 0 else (theirs_in, mine_in)
        for i, half in enumerate(halves):
            white[:, i * LANES : (i + 1) * LANES] = half[SECOND:, :]

    core = lax.axis_index("rep")

    @pl.when(core == 0)
    def _():
        write(0, 2 * PART, 3 * PART)

    @pl.when(core == 1)
    def _():
        write(2 * PART, 0, PART)

    sums = joined(mine_in[:SECOND, :])
    proj[...] = laid([(sums, OWN + 1, 0), (sums, OWN2 + 1, PART)])[:1, : 2 * PART]


def vmem(n):
    return [pl.BlockSpec(memory_space=pltpu.VMEM)] * n


HBM = pl.BlockSpec(memory_space=pltpu.HBM)
SWAP = [(0, 1), (1, 0)]


def stay(a):
    return pltpu.with_memory_space_constraint(a, pltpu.HBM)


def near_by(a):
    return pltpu.with_memory_space_constraint(a, pltpu.VMEM)


def shards(
    residual, toa_error, basis_rows, efac_table, equad_table, pulsar, backend, counts, owner_slot
):
    far, near = lax.axis_size(FAR), lax.axis_size(NEAR)
    tiles, cols, rows = basis_rows.shape
    own = jnp.transpose(basis_rows, (1, 0, 2))
    other = lax.ppermute(own, "rep", SWAP)
    block = far + far * WIDE
    message = message_rows(far)
    line = lambda a: a.reshape(1, -1)
    ints = [line(a) for a in (pulsar, backend, counts, owner_slot)]
    left, acc = pl.pallas_call(
        functools.partial(own_kernel, near, far),
        out_shape=(
            jax.ShapeDtypeStruct((tiles, 2 * SECOND, rows), BF16),
            jax.ShapeDtypeStruct((near * block + 8, LANES), F32),
        ),
        in_specs=[HBM] * 9,
        out_specs=tuple(vmem(2)),
        scratch_shapes=[pltpu.VMEM((1, tiles), jnp.int32)] * 4
        + [pltpu.VMEM((tiles, rows), F32)] * 2
        + [pltpu.VMEM(efac_table.shape[::-1], F32)] * 2
        + [
            pltpu.VMEM(own.shape, BF16),
            pltpu.SMEM((1, tiles), jnp.int32),
            pltpu.VMEM((tiles, rows), F32),
            pltpu.VMEM((tiles, rows), BF16),
            pltpu.SemaphoreType.DMA((9,)),
            pltpu.SemaphoreType.DMA((tiles // GROUP,)),
        ],
        compiler_params=pltpu.CompilerParams(vmem_limit_bytes=32 << 20),
        cost_estimate=pl.CostEstimate(flops=2 * 10**9, transcendentals=0, bytes_accessed=10**7),
        name="own",
    )(*map(stay, (*ints, residual, toa_error, efac_table.T, equad_table.T, own)))
    sent, _ = pl.pallas_call(
        functools.partial(cross_kernel, near, far),
        out_shape=(
            pltpu.VMEM((near, message, LANES), BF16),
            pltpu.VMEM((near * block + 8, LANES), F32),
        ),
        in_specs=vmem(4),
        out_specs=tuple(vmem(2)),
        input_output_aliases={2: 1},
        compiler_params=pltpu.CompilerParams(vmem_limit_bytes=32 << 20),
        name="cross",
    )(ints[0], left, acc, other)
    got = lax.all_to_all(sent, NEAR, 0, 0, tiled=True)
    sent = pl.pallas_call(
        functools.partial(near_kernel, far),
        out_shape=pltpu.VMEM((far, WHITE + SECOND, LANES), BF16),
        in_specs=vmem(1),
        out_specs=vmem(1)[0],
        scratch_shapes=[pltpu.VMEM((message, LANES), F32)],
        name="near_sum",
    )(near_by(got))
    got = lax.all_to_all(sent, FAR, 0, 0, tiled=True)
    mine = pl.pallas_call(
        far_kernel,
        out_shape=pltpu.VMEM((SECOND + tiles, LANES), F32),
        in_specs=vmem(1),
        out_specs=vmem(1)[0],
        name="far_sum",
    )(near_by(got))
    theirs = lax.ppermute(mine, "rep", SWAP)
    gram, projection, whitened = pl.pallas_call(
        join_kernel,
        out_shape=(
            jax.ShapeDtypeStruct((cols, 1, 2 * cols), F32),
            jax.ShapeDtypeStruct((1, cols), F32),
            jax.ShapeDtypeStruct((tiles, rows), F32),
        ),
        in_specs=vmem(2),
        out_specs=tuple(vmem(3)),
        scratch_shapes=[pltpu.VMEM((LANES, LANES), F32)] * 2,
        name="join",
    )(near_by(mine), near_by(theirs))
    return jnp.transpose(gram, (1, 2, 0)), projection, whitened


def solution(mesh):
    split = Mesh(
        mesh.devices.reshape(8, 4, 4, mesh.shape["rep"]), ("toa_0", "toa_1", "toa_2", "rep")
    )
    placed = (
        P(TOA, None),
        P(TOA, None),
        P(TOA, "rep", None),
        P(),
        P(),
        P(TOA),
        P(TOA),
        P(TOA),
        P(TOA),
    )
    return jax.shard_map(
        shards,
        mesh=split,
        in_specs=placed,
        out_specs=(P(TOA, None, "rep"), P(TOA, "rep"), P(TOA, None)),
        check_vma=False,
    )
```

```python
import functools

import jax
import jax.numpy as jnp
from jax import lax
from jax.experimental import pallas as pl
from jax.experimental.pallas import tpu as pltpu
from jax.sharding import Mesh
from jax.sharding import PartitionSpec as P

TOA = ("toa_0", "toa_1", "toa_2")
FAR, NEAR = "toa_0", ("toa_1", "toa_2")
BF16, F32 = jnp.bfloat16, jnp.float32
LANES = 128
GROUP = 16

PART = 25
WIDE = PART + 1
SECOND = 32
OWN = 2 * PART
OWN2 = OWN + SECOND
USED = OWN2 + WIDE
PIECE = 18
PLACE = 126
LAST_PLACE = 124
WHITE = 16


def dot(a, b, dims=((1,), (0,)), **kw):
    return lax.dot_general(a, b, (dims, ((), ())), preferred_element_type=F32, **kw)


def iota(shape, dim):
    return lax.broadcasted_iota(jnp.int32, shape, dim)


def as_column(row, lanes):
    square = jnp.broadcast_to(row, (LANES, row.shape[1])).T
    return jnp.concatenate([square] * (lanes // LANES), axis=1)


def base_row(p, near, message, head):
    return (p & (near - 1)) * message + head + (p >> (near.bit_length() - 1)) * WIDE


def split(value):
    lane = iota(value.shape, 1)
    rest = value - value.astype(BF16).astype(F32)
    first = pltpu.roll(rest, LANES - OWN - 1, 1)
    second = pltpu.roll(rest, LANES - (OWN2 + 1 - PART), 1)
    return jnp.where(lane < PART, first, jnp.where(lane < OWN, second, value))


def joined(value):
    lane = iota(value.shape, 1)
    first = pltpu.roll(value, OWN + 1, 1)
    second = pltpu.roll(value, OWN2 + 1 - PART, 1)
    return value + jnp.where(lane < OWN2, first, second)


def message_rows(far):
    rows = far + (far - 1) * WIDE
    return rows + -rows % 8


def own_kernel(
    near, far, pulsar_in, backend_in, counts_in, slot_in, residual_in, error_in, efac_in, equad_in,
    own_in, left_out, acc,
    pulsar, backend, counts, slot, residual, error, efac_t, equad_t, own, pulsar_sm,
    weight_vm, wres_vm, sems, own_sems,
):
    cols, tiles, rows = own.shape
    block = far + far * WIDE
    pulsars, backends = efac_t.shape[1], efac_t.shape[0]
    pairs = (
        (pulsar_in, pulsar), (backend_in, backend), (efac_in, efac_t), (equad_in, equad_t),
        (counts_in, counts), (error_in, error), (residual_in, residual), (slot_in, slot),
        (pulsar_in, pulsar_sm),
    )
    copies = [pltpu.make_async_copy(a, b, sems.at[i]) for i, (a, b) in enumerate(pairs)]

    def own_copy(g):
        here = pl.ds(pl.multiple_of(g * GROUP, GROUP), GROUP)
        return pltpu.make_async_copy(own_in.at[:, here, :], own.at[:, here, :], own_sems.at[g])

    for copy in copies:
        copy.start()
    for g in range(tiles // GROUP):
        own_copy(g).start()
    acc[...] = jnp.zeros_like(acc)
    for copy in copies[:4]:
        copy.wait()

    of_pulsar = (iota((pulsars, tiles), 0) == pulsar[...]).astype(F32)
    of_backend = (iota((backends, tiles), 0) == backend[...]).astype(F32)
    high = dict(precision=lax.Precision.HIGHEST)
    factor = jnp.sum(dot(efac_t[...], of_pulsar, **high) * of_backend, axis=0, keepdims=True)
    floor = jnp.sum(dot(equad_t[...], of_pulsar, **high) * of_backend, axis=0, keepdims=True)
    factor2 = as_column(factor * factor, rows)
    floor2 = as_column(floor * floor, rows)
    for copy in copies[4:7]:
        copy.wait()
    count = as_column(counts[...].astype(F32), rows)
    valid = iota((tiles, rows), 1).astype(F32) < count
    weight = jnp.where(valid, 1.0 / (factor2 * error[...] ** 2 + floor2), 0.0)
    weight_vm[...] = weight
    wres_vm[...] = (weight * residual[...]).astype(BF16)
    white = jnp.sqrt(weight) * residual[...]
    white = jnp.where(lax.axis_index("rep") == 0, white[:, :LANES], white[:, LANES:])

    me = lax.axis_index("toa_1") * lax.axis_size("toa_2") + lax.axis_index("toa_2")
    copies[7].wait()
    dest = slot[...] // tiles
    place = (slot[...] % tiles).astype(F32)
    order = (dest % near) * far + dest // near
    moved = (iota((tiles, tiles), 0) == order).astype(BF16)
    white_to = dot(moved, white.astype(BF16))
    place_to = dot(moved, as_column(place, LANES).astype(BF16))
    place_to = jnp.where(iota(place_to.shape, 1) == PLACE, place_to, 0.0)
    for n in range(near):
        at = n * block
        acc[at : at + far, :] = white_to[n * far : (n + 1) * far, :]
        acc[pl.ds(at + far + me, far, stride=WIDE), :] = place_to[n * far : (n + 1) * far, :]

    copies[8].wait()

    lefts = 2 * SECOND
    lane, row = iota((SECOND, lefts), 1), iota((SECOND, lefts), 0)
    lower = (row > 0) & (lane < row) & (lane < PART)
    projected = row == 0
    is_wres = iota((GROUP, rows), 0) == 0
    beyond = jnp.zeros((SECOND, SECOND + 1), F32)

    def turn(g, carry):
        t0 = pl.multiple_of(g * GROUP, GROUP)
        here = pl.ds(t0, GROUP)
        own_copy(g).wait()
        none = lambda n: jnp.zeros((n, GROUP, rows), BF16)
        slabs = [
            none(1),
            own[:PART, here, :],
            none(SECOND - WIDE),
            wres_vm[here, :].reshape(1, GROUP, rows),
            own[PART:, here, :],
            none(SECOND - WIDE),
        ]
        turned = pltpu.einshape("ktr->tkr", jnp.concatenate(slabs, axis=0))
        group_weight = weight_vm[here, :]
        for u in range(GROUP):
            right = turned[u]
            left = (right.astype(F32) * group_weight[u : u + 1, :]).astype(BF16)
            middle = slice(SECOND, SECOND + GROUP)
            middle = jnp.where(is_wres, right[middle], left[middle])
            left = jnp.concatenate([left[:SECOND], middle, left[SECOND + GROUP :]], axis=0)
            left_out[t0 + u] = left
            out = dot(left, right, ((1,), (1,)))
            low, high = out[:SECOND], out[SECOND:]
            moved = jnp.concatenate([high[:, SECOND + 1 :], beyond], axis=1)
            value = jnp.where(lower, moved, jnp.where(projected, high, low))
            base = base_row(pulsar_sm[0, t0 + u], near, block, far)
            acc[pl.ds(base, WIDE), OWN:USED] += value[:WIDE, : USED - OWN]
        return carry

    lax.fori_loop(0, tiles // GROUP, turn, 0)
    for n in range(near):
        here = pl.ds(n * block + far, far, stride=WIDE)
        acc[here, :] = split(acc[here, :])


def cross_kernel(near, far, pulsar, left, acc_in, other, out, acc):
    cols, tiles, rows = other.shape
    block = far + far * WIDE
    message = out.shape[1]
    core = lax.axis_index("rep")
    lane, row = iota((SECOND, cols), 1), iota((SECOND, cols), 0)
    second = (lane >= PART) & (row > 0)
    bases = base_row(pulsar[...], near, block, far).astype(F32)
    tile = iota(bases.shape, 1)

    def turn(g, carry):
        t0 = pl.multiple_of(g * GROUP, GROUP)
        here = pl.ds(t0, GROUP)
        slabs = [other[pl.ds(PART * core, PART), here, :], other[pl.ds(PART - PART * core, PART), here, :]]
        turned = pltpu.einshape("ktr->tkr", jnp.concatenate(slabs, axis=0))
        for u in range(GROUP):
            product = dot(left[t0 + u], turned[u], ((1,), (1,)))
            value = jnp.where(second, product[SECOND:], product[:SECOND])
            base = jnp.sum(jnp.where(tile == t0 + u, bases, 0.0)).astype(jnp.int32)
            acc[pl.ds(base, WIDE), :cols] += value[:WIDE]
        return carry

    lax.fori_loop(0, tiles // GROUP, turn, 0, unroll=tiles // GROUP)

    lane = iota((WIDE, LANES), 1)
    spare = (lane >= USED) & (lane < USED + PIECE)

    def fold(n, carry):
        at = n * block + far
        last = acc[pl.ds(at + (far - 1) * WIDE, SECOND), :].astype(BF16)
        for i in range(far - 1):
            here = acc.at[pl.ds(at + i * WIDE, WIDE), :]
            if i < USED // PIECE:
                pltpu.store(here, pltpu.roll(last, USED - i * PIECE, 1).astype(F32)[:WIDE], mask=spare)
            else:
                place = pltpu.roll(last, LANES - (PLACE - LAST_PLACE), 1).astype(F32)[:WIDE]
                pltpu.store(here, place, mask=lane == LAST_PLACE)
        return carry

    def convert(n, carry):
        out[n] = acc[pl.ds(pl.multiple_of(n * block, 8), message), :].astype(BF16)
        return carry

    lax.fori_loop(0, near, fold, 0, unroll=8)
    lax.fori_loop(0, near, convert, 0, unroll=4)


def near_kernel(far, got, out, total):
    near = got.shape[0]
    part = got[:, :far, :].astype(F32)
    out[:, :near, :] = jnp.swapaxes(part, 0, 1).astype(BF16)
    summed = got[0, far:, :].astype(F32)
    for n in range(1, near):
        summed = summed + got[n, far:, :].astype(F32)
    total[: summed.shape[0], :] = summed
    total[summed.shape[0] :, :] = jnp.zeros((total.shape[0] - summed.shape[0], LANES), F32)
    lane, row = iota((SECOND, LANES), 1), iota((SECOND, LANES), 0)
    last = jnp.zeros((SECOND, LANES), F32)
    for f in range(far):
        if f < far - 1:
            block = total[f * WIDE : f * WIDE + SECOND, :]
            if f < USED // PIECE:
                moved = pltpu.roll(block, LANES - (USED - f * PIECE), 1)
                last = jnp.where((lane >= f * PIECE) & (lane < (f + 1) * PIECE), moved, last)
            else:
                last = jnp.where(lane == PLACE, pltpu.roll(block, PLACE - LAST_PLACE, 1), last)
        else:
            block = last
        whole = split(joined(block))
        whole = jnp.where(lane == PLACE, block, whole)
        out[f, WHITE:, :] = jnp.where(row == 0, whole, block).astype(BF16)


def far_kernel(got, out):
    far, near = got.shape[0], WHITE
    tiles = far * near
    total = got[0, WHITE:, :].astype(F32)
    for f in range(1, far):
        total = total + got[f, WHITE:, :].astype(F32)
    out[:SECOND, :] = total
    lane = iota((near, LANES), 1)
    puts = []
    for f in range(far):
        value = got[f, WHITE : WHITE + near, :].astype(F32)
        place = jnp.sum(jnp.where(lane == PLACE, value, 0.0), axis=1, keepdims=True)
        puts.append((lane.astype(F32) == place).astype(F32))
    put = jnp.concatenate(puts, axis=0).astype(BF16)
    out[SECOND:, :] = dot(put, got[:, :near, :].reshape(tiles, LANES), ((0,), (0,)))


def join_kernel(mine_in, theirs_in, gram, proj, white, mine_t, theirs_t, sems):
    core = lax.axis_index("rep")
    copies = []
    for i, (half, at) in enumerate(((mine_in, core), (theirs_in, 1 - core))):
        to = white.at[:, pl.ds(pl.multiple_of(at * LANES, LANES), LANES)]
        copies.append(pltpu.make_async_copy(half.at[SECOND:, :], to, sems.at[i]))
        copies[-1].start()
    lane, row = iota((SECOND, LANES), 1), iota((SECOND, LANES), 0)
    mine = mine_in[1 : SECOND + 1, :]

    def square(a):
        return jnp.concatenate([a, jnp.zeros((LANES - SECOND, LANES), F32)], axis=0).T

    mine_t[...] = square(mine)
    theirs_t[...] = square(theirs_in[1 : SECOND + 1, :])
    low = pltpu.roll(mine, LANES - OWN - 1, 1)
    first = jnp.where(lane >= row, low, mine_t[OWN + 1 : OWN + SECOND + 1, :])
    high = pltpu.roll(mine, LANES - OWN, 1)
    second = jnp.where(lane <= row, high, mine_t[OWN : OWN + SECOND, :])
    turned = mine_t[OWN2 + 1 : OWN2 + SECOND + 1, :]
    theirs_0 = theirs_t[:SECOND, :]
    theirs_1 = theirs_t[PART : PART + SECOND, :]

    def laid(pieces):
        value = jnp.zeros((SECOND, LANES), F32)
        for source, start, to in pieces:
            moved = pltpu.roll(source, (to - start) % LANES, 1) if to != start else source
            value = jnp.where((lane >= to) & (lane < to + PART), moved, value)
        return value

    def write(own, low, high):
        top = [(first, 0, own), (mine, OWN2 + 1, own + PART)]
        under = [(turned, 0, own), (second, 0, own + PART)]
        if own == 0:
            top += [(mine, 0, low), (theirs_1, 0, high)]
            under += [(theirs_0, 0, low), (mine, PART, high)]
        else:
            top += [(theirs_0, 0, low), (mine, 0, high)]
            under += [(mine, PART, low), (theirs_1, 0, high)]
        gram[:PART, 0, :] = laid(top)[:PART, : 4 * PART]
        gram[PART:, 0, :] = laid(under)[:PART, : 4 * PART]

    @pl.when(core == 0)
    def _():
        write(0, 2 * PART, 3 * PART)

    @pl.when(core == 1)
    def _():
        write(2 * PART, 0, PART)

    sums = joined(mine_in[:SECOND, :])
    proj[...] = laid([(sums, OWN + 1, 0), (sums, OWN2 + 1, PART)])[:1, : 2 * PART]
    for copy in copies:
        copy.wait()


def vmem(n):
    return [pl.BlockSpec(memory_space=pltpu.VMEM)] * n


HBM = pl.BlockSpec(memory_space=pltpu.HBM)
SWAP = [(0, 1), (1, 0)]


def stay(a):
    return pltpu.with_memory_space_constraint(a, pltpu.HBM)


def near_by(a):
    return pltpu.with_memory_space_constraint(a, pltpu.VMEM)


def shards(
    residual, toa_error, basis_rows, efac_table, equad_table, pulsar, backend, counts, owner_slot
):
    far, near = lax.axis_size(FAR), lax.axis_size(NEAR)
    tiles, cols, rows = basis_rows.shape
    own = jnp.transpose(basis_rows, (1, 0, 2))
    other = lax.ppermute(own, "rep", SWAP)
    block = far + far * WIDE
    message = message_rows(far)
    line = lambda a: a.reshape(1, -1)
    ints = [line(a) for a in (pulsar, backend, counts, owner_slot)]
    left, acc = pl.pallas_call(
        functools.partial(own_kernel, near, far),
        out_shape=(
            jax.ShapeDtypeStruct((tiles, 2 * SECOND, rows), BF16),
            jax.ShapeDtypeStruct((near * block + 8, LANES), F32),
        ),
        in_specs=[HBM] * 9,
        out_specs=tuple(vmem(2)),
        scratch_shapes=[pltpu.VMEM((1, tiles), jnp.int32)] * 4
        + [pltpu.VMEM((tiles, rows), F32)] * 2
        + [pltpu.VMEM(efac_table.shape[::-1], F32)] * 2
        + [
            pltpu.VMEM(own.shape, BF16),
            pltpu.SMEM((1, tiles), jnp.int32),
            pltpu.VMEM((tiles, rows), F32),
            pltpu.VMEM((tiles, rows), BF16),
            pltpu.SemaphoreType.DMA((9,)),
            pltpu.SemaphoreType.DMA((tiles // GROUP,)),
        ],
        compiler_params=pltpu.CompilerParams(vmem_limit_bytes=32 << 20),
        cost_estimate=pl.CostEstimate(flops=2 * 10**9, transcendentals=0, bytes_accessed=10**7),
        name="own",
    )(*map(stay, (*ints, residual, toa_error, efac_table.T, equad_table.T, own)))
    sent, _ = pl.pallas_call(
        functools.partial(cross_kernel, near, far),
        out_shape=(
            pltpu.VMEM((near, message, LANES), BF16),
            pltpu.VMEM((near * block + 8, LANES), F32),
        ),
        in_specs=vmem(4),
        out_specs=tuple(vmem(2)),
        input_output_aliases={2: 1},
        compiler_params=pltpu.CompilerParams(vmem_limit_bytes=32 << 20),
        name="cross",
    )(ints[0], left, acc, other)
    got = lax.all_to_all(sent, NEAR, 0, 0, tiled=True)
    sent = pl.pallas_call(
        functools.partial(near_kernel, far),
        out_shape=pltpu.VMEM((far, WHITE + SECOND, LANES), BF16),
        in_specs=vmem(1),
        out_specs=vmem(1)[0],
        scratch_shapes=[pltpu.VMEM((message, LANES), F32)],
        name="near_sum",
    )(near_by(got))
    got = lax.all_to_all(sent, FAR, 0, 0, tiled=True)
    mine = pl.pallas_call(
        far_kernel,
        out_shape=pltpu.VMEM((SECOND + tiles, LANES), F32),
        in_specs=vmem(1),
        out_specs=vmem(1)[0],
        name="far_sum",
    )(near_by(got))
    theirs = lax.ppermute(mine, "rep", SWAP)
    gram, projection, whitened = pl.pallas_call(
        join_kernel,
        out_shape=(
            jax.ShapeDtypeStruct((cols, 1, 2 * cols), F32),
            jax.ShapeDtypeStruct((1, cols), F32),
            jax.ShapeDtypeStruct((tiles, rows), F32),
        ),
        in_specs=vmem(2),
        out_specs=tuple(vmem(2) + [HBM]),
        scratch_shapes=[pltpu.VMEM((LANES, LANES), F32)] * 2 + [pltpu.SemaphoreType.DMA((2,))],
        name="join",
    )(near_by(mine), near_by(theirs))
    return jnp.transpose(gram, (1, 2, 0)), projection, whitened


def solution(mesh):
    split = Mesh(
        mesh.devices.reshape(8, 4, 4, mesh.shape["rep"]), ("toa_0", "toa_1", "toa_2", "rep")
    )
    placed = (
        P(TOA, None),
        P(TOA, None),
        P(TOA, "rep", None),
        P(),
        P(),
        P(TOA),
        P(TOA),
        P(TOA),
        P(TOA),
    )
    return jax.shard_map(
        shards,
        mesh=split,
        in_specs=placed,
        out_specs=(P(TOA, None, "rep"), P(TOA, "rep"), P(TOA, None)),
        check_vma=False,
    )
```
